32 devices in a mesh: lat: 16 (over z, x, core), lon: 2 (over y).
Axes of the slice: x: 2, y: 2, z: 4, core: 2. Of those that a mesh axis runs over, the one named last changes fastest.
Arguments:
- elevation: float32 [4096, 4096], P('lat', 'lon'), may hold values from -200 to 200
Outputs:
- slope_angle: float32 [4096, 4096], P('lat', 'lon')
- facing: float32 [2, 4096, 4096], P(None, 'lat', 'lon')
- hillshade: float32 [4096, 4096], P('lat', 'lon')
The draws below stay inside these ranges and needn't reach their ends.
All inputs are finite; a program needn't handle non-finite values.
Results may differ from the reference program's by a relative error of at most 0.0003.
Values sent between devices are 32-bit elements; how exact they have to be, the bound alone decides.
A program may use at most 64 MiB of HBM per device.

```python
import math
import jax
import jax.numpy as jnp
from jax import lax

SCALES = 7
HALO = 64
NROWS = 4096
NCOLS = 4096


def draw_elevation(key, part):
    surface = jnp.zeros((NROWS, NCOLS), jnp.float32)
    for octave in range(SCALES):
        stride = 2 ** octave
        noise_key = jax.random.fold_in(key, 11 + octave)
        shift_key = jax.random.fold_in(key, 101 + octave)
        coarse_shape = (NROWS // stride, NCOLS // stride)
        coarse = jax.random.truncated_normal(noise_key, -4.0, 4.0, coarse_shape, jnp.float32)
        amplitude = 2.0 * math.sqrt(stride)
        upsampled = jnp.repeat(jnp.repeat(coarse, stride, axis=0), stride, axis=1)
        offsets = jax.random.randint(shift_key, (2,), 0, stride)
        upsampled = jnp.roll(upsampled, (offsets[0], offsets[1]), axis=(0, 1))
        surface = surface + amplitude * upsampled
    return surface


def setup_inputs(seed: int = 0) -> dict:
    streams_of = jax.random.split(jax.random.key(seed), 2)
    elevation = draw_elevation(jax.random.fold_in(streams_of[1], 71), 0)
    return dict(elevation=elevation)


LIGHT_EAST = -0.5
LIGHT_NORTH = 0.5
LIGHT_UP = math.sqrt(0.5)

def window(padded, margin, row_offset, col_offset, row_count, col_count):
    return lax.slice(padded, (margin + row_offset, margin + col_offset), (margin + row_offset + row_count, margin + col_offset + col_count))

def terrain_shading(padded, spacing, margin, levels):
    row_count = padded.shape[0] - 2 * margin
    col_count = padded.shape[1] - 2 * margin
    eastward = jnp.zeros((row_count, col_count), jnp.float32)
    northward = jnp.zeros((row_count, col_count), jnp.float32)
    for octave in range(levels):
        stride = 2 ** octave
        north_west = window(padded, margin, -stride, -stride, row_count, col_count)
        north_mid = window(padded, margin, -stride, 0, row_count, col_count)
        north_east = window(padded, margin, -stride, stride, row_count, col_count)
        west_mid = window(padded, margin, 0, -stride, row_count, col_count)
        east_mid = window(padded, margin, 0, stride, row_count, col_count)
        south_west = window(padded, margin, stride, -stride, row_count, col_count)
        south_mid = window(padded, margin, stride, 0, row_count, col_count)
        south_east = window(padded, margin, stride, stride, row_count, col_count)
        east_diff = north_east + 2.0 * east_mid + south_east - (north_west + 2.0 * west_mid + south_west)
        north_diff = north_west + 2.0 * north_mid + north_east - (south_west + 2.0 * south_mid + south_east)
        eastward = eastward + east_diff * (1.0 / stride)
        northward = northward + north_diff * (1.0 / stride)
    grad_east = eastward / (8.0 * levels * spacing[:, None])
    grad_north = northward * (1.0 / (8.0 * levels))
    squared = grad_east * grad_east + grad_north * grad_north
    slope_angle = jnp.arctan(jnp.sqrt(squared))
    inverse = lax.rsqrt(1.0 + squared)
    facing_east = -grad_east * inverse
    facing_north = -grad_north * inverse
    shading = jnp.maximum(LIGHT_EAST * facing_east + LIGHT_NORTH * facing_north + LIGHT_UP * inverse, 0.0)
    return (slope_angle, jnp.stack([facing_east, facing_north]), shading)

def reference(elevation):
    margin = HALO
    wrapped = jnp.concatenate([elevation[:, NCOLS - margin:], elevation, elevation[:, :margin]], axis=1)
    padded = jnp.concatenate([jnp.broadcast_to(wrapped[:1], (margin, NCOLS + 2 * margin)), wrapped, jnp.broadcast_to(wrapped[NROWS - 1:], (margin, NCOLS + 2 * margin))], axis=0)
    position = jnp.arange(NROWS, dtype=jnp.int32)
    spacing = jnp.sin((position.astype(jnp.float32) + 0.5) * (math.pi / NROWS)) * (2.0 * NROWS / NCOLS)
    block_rows = math.gcd(NROWS, 512)
    block_count = NROWS // block_rows

    def one_block(number):
        first_row = (number * block_rows).astype(jnp.int32)
        slab = lax.dynamic_slice(padded, (first_row, jnp.int32(0)), (block_rows + 2 * margin, NCOLS + 2 * margin))
        slab_spacing = lax.dynamic_slice(spacing, (first_row,), (block_rows,))
        return terrain_shading(slab, slab_spacing, margin, SCALES)
    results = lax.map(one_block, jnp.arange(block_count, dtype=jnp.int32))
    slope_angle = results[0].reshape(NROWS, NCOLS)
    facing = jnp.transpose(results[1], (1, 0, 2, 3)).reshape(2, NROWS, NCOLS)
    hillshade = results[2].reshape(NROWS, NCOLS)
    return (slope_angle, facing, hillshade)
```

```python
import functools
import math

import jax
import jax.numpy as jnp
from jax import lax
from jax.experimental import pallas as pl
from jax.experimental.pallas import tpu as pltpu
from jax.sharding import PartitionSpec as P

SCALES = 7
HALO = 64
LANES = 128
SUB = 8
RUNS = 2

LIGHT_UP = math.sqrt(0.5)
MESH = pl.DeviceIdType.MESH

ANGLE = (
    1.5707962050889646,
    -0.9999801696091738,
    0.7848538132927688,
    -0.6607586188432167,
    0.5557489578459907,
    -0.42189571811945836,
    0.2501265286961767,
    -0.09607630454800326,
    0.01718536914918157,
)


def row_pad(octave):
    return max(2**octave, SUB)


def near_side(lat):
    return 1 - lax.rem(lat, 2)


def fill_coef(coef_ref, count, first_row, total_rows, total_cols):
    for start in range(0, count, SUB):
        position = first_row + start + lax.broadcasted_iota(jnp.int32, (SUB, LANES), 0)
        spacing = jnp.sin((position.astype(jnp.float32) + 0.5) * (math.pi / total_rows)) * (
            2.0 * total_rows / total_cols
        )
        coef_ref[pl.ds(start, SUB), :] = 1.0 / (8.0 * SCALES * spacing)


class Window:
    def __init__(self, strips, base, count, width, boxes, sums, coef, slope, facing, shade):
        self.strips, self.base, self.count, self.width = strips, base, count, width
        self.boxes, self.sums, self.coef = boxes, sums, coef
        self.slope, self.facing, self.shade = slope, facing, shade
        self.lane = lax.broadcasted_iota(jnp.int32, (SUB, LANES), 1)

    def here(self, starts, row):
        top = pl.multiple_of(self.base + row, SUB)
        return [
            [self.strips[start + k, pl.ds(top, SUB), :] for k in range(self.width + 2)]
            for start in starts
        ]

    def box(self, starts, row, octave, here):
        lag = 2**octave
        top = pl.multiple_of(self.base + row, SUB)
        boxes, shifted = [], []
        for start, z in zip(starts, here):
            pair = []
            for k in range(self.width + 2):
                total = z[k] + self.strips[start + k, pl.ds(top + lag, SUB), :]
                pair.append(total * (1.0 / lag) if octave else total)
            ahead = [pltpu.roll(v, LANES - lag, 1) for v in pair]
            if 2 * lag == LANES:
                plus = [
                    jnp.where(self.lane < lag, ahead[k], ahead[k + 1])
                    for k in range(self.width + 1)
                ]
                boxes += [pair[k + 1] + plus[k + 1] for k in range(self.width)]
                shifted += [pair[k + 1] + plus[k] for k in range(self.width)]
            else:
                behind = [pltpu.roll(v, lag, 1) for v in pair]
                for k in range(1, self.width + 1):
                    plus = jnp.where(self.lane < LANES - lag, ahead[k], ahead[k + 1])
                    minus = jnp.where(self.lane >= lag, behind[k], behind[k - 1])
                    boxes.append(pair[k] + plus)
                    shifted.append(pair[k] + minus)
        return boxes, shifted

    def keep(self, row, octave, boxes, shifted):
        place = pl.ds(pl.multiple_of(row + row_pad(octave), SUB), SUB)
        for k in range(RUNS * self.width):
            self.boxes[octave][0, k, place, :] = boxes[k]
            self.boxes[octave][1, k, place, :] = shifted[k]

    def before(self, starts):
        for distance in range(SUB, HALO + SUB, SUB):
            here = self.here(starts, -distance)
            for octave in range(SCALES):
                if row_pad(octave) >= distance:
                    boxes, shifted = self.box(starts, -distance, octave, here)
                    self.keep(-distance, octave, boxes, shifted)

    def add(self, starts, row):
        here = self.here(starts, row)
        first = second = None
        for octave in range(SCALES):
            boxes, shifted = self.box(starts, row, octave, here)
            self.keep(row, octave, boxes, shifted)
            past = pl.ds(row + row_pad(octave) - 2**octave, SUB)
            u = [boxes[k] - self.boxes[octave][1, k, past, :] for k in range(RUNS * self.width)]
            v = [self.boxes[octave][0, k, past, :] - shifted[k] for k in range(RUNS * self.width)]
            first = u if first is None else [a + b for a, b in zip(first, u)]
            second = v if second is None else [a + b for a, b in zip(second, v)]
        return first, second

    def hold(self, first, second):
        for k in range(RUNS * self.width):
            self.sums[0, k] = first[k]
            self.sums[1, k] = second[k]

    def held(self):
        count = RUNS * self.width
        return [self.sums[0, k] for k in range(count)], [self.sums[1, k] for k in range(count)]

    def finish(self, starts, row, first, second):
        rows = pl.ds(row, SUB)
        coef = self.coef[rows, :]
        for k in range(RUNS * self.width):
            run, within = divmod(k, self.width)
            column = pl.ds(pl.multiple_of((starts[run] + within) * LANES, LANES), LANES)
            grad_east = (first[k] + second[k]) * coef
            grad_north = (second[k] - first[k]) * (1.0 / (8.0 * SCALES))
            squared = grad_east * grad_east + grad_north * grad_north
            inverse = lax.rsqrt(1.0 + squared)
            sine = squared * lax.rsqrt(jnp.maximum(squared, 1e-37)) * inverse
            ratio = jnp.full_like(inverse, ANGLE[-1])
            for term in ANGLE[-2::-1]:
                ratio = ratio * inverse + term
            self.slope[rows, column] = sine * ratio
            self.facing[0, rows, column] = -grad_east * inverse
            self.facing[1, rows, column] = -grad_north * inverse
            tilt = 0.5 * (grad_east - grad_north) + LIGHT_UP
            self.shade[rows, column] = jnp.maximum(tilt * inverse, 0.0)

    def run(self, starts):
        self.before(starts)
        self.hold(*self.add(starts, 0))

        def step(number, carry):
            row = pl.multiple_of(number * SUB, SUB)
            first, second = self.held()
            sums = self.add(starts, row)
            self.finish(starts, pl.multiple_of(row - SUB, SUB), first, second)
            self.hold(*sums)
            return carry

        lax.fori_loop(1, self.count // SUB, step, 0)
        self.finish(starts, self.count - SUB, *self.held())


def run_starts(half, strips):
    quarter = strips // 4
    return (
        jnp.where(half == 0, quarter, 0),
        jnp.where(half == 0, 2 * quarter, 3 * quarter),
    )


def gather(rows, cols, z_ref, strips_ref, slope, facing, shade, *scratch):
    boxes, (sums, coef, load_sem, send_sem, recv_sem, rim_send, rim_recv) = (
        scratch[:SCALES],
        scratch[SCALES:],
    )
    lat, lon = lax.axis_index("lat"), lax.axis_index("lon")
    n_lat, n_lon = lax.axis_size("lat"), lax.axis_size("lon")
    west, east = lax.rem(lon + n_lon - 1, n_lon), lax.rem(lon + 1, n_lon)
    strips = cols // LANES
    near = near_side(lat)
    far = 1 - near
    exists = (lat > 0, lat < n_lat - 1)
    far_exists = jnp.where(far == 0, exists[0], exists[1])
    far_lat = jnp.where(far == 0, lat - 1, lat + 1)
    near_lat = jnp.where(near == 0, lat - 1, lat + 1)

    def edge(side):
        return pl.multiple_of(jnp.where(side == 0, 0, rows - HALO), SUB)

    def halo(side):
        return pl.multiple_of(jnp.where(side == 0, 0, HALO + rows), SUB)

    def loads_of(number):
        start, count = ((edge(far), HALO), (edge(near), HALO), (HALO, rows - 2 * HALO))[number]
        return [
            pltpu.make_async_copy(
                z_ref.at[pl.ds(start, count), pl.ds(strip * LANES, LANES)],
                strips_ref.at[1 + strip, pl.ds(HALO + start, count), :],
                load_sem.at[number, strip],
            )
            for strip in range(strips)
        ]

    for number in range(3):
        for load in loads_of(number):
            load.start()

    barrier = pltpu.get_barrier_semaphore()

    @pl.when(far_exists)
    def _():
        for other in (lon, west, east):
            pl.semaphore_signal(barrier, inc=1, device_id=(far_lat, other), device_id_type=MESH)

    for other in (west, east):
        pl.semaphore_signal(barrier, inc=1, device_id=(lat, other), device_id_type=MESH)
    for other in (lon, west, east):
        pl.semaphore_signal(barrier, inc=1, device_id=(near_lat, other), device_id_type=MESH)

    main = rows - HALO
    base = pl.multiple_of(jnp.where(far == 0, HALO, 0), SUB)
    fill_coef(coef, main, lat * rows + base, rows * n_lat, cols * n_lon)
    pl.semaphore_wait(barrier, 5 + 3 * far_exists.astype(jnp.int32))

    def lat_copy(distant, kind):
        side, other = (far, far_lat) if distant else (near, near_lat)
        source, target, count, other_lon = (
            (1, 1, strips, lon),
            (1, strips + 1, 1, west),
            (strips, 0, 1, east),
        )[kind]
        return pltpu.make_async_remote_copy(
            src_ref=strips_ref.at[pl.ds(source, count), pl.ds(HALO + edge(side), HALO), :],
            dst_ref=strips_ref.at[pl.ds(target, count), pl.ds(halo(1 - side), HALO), :],
            send_sem=send_sem.at[distant, kind],
            recv_sem=recv_sem.at[distant, kind],
            device_id=(other, other_lon),
            device_id_type=MESH,
        )

    def rim_copy(side):
        source, target, other = ((1, strips + 1, west), (strips, 0, east))[side]
        return pltpu.make_async_remote_copy(
            src_ref=strips_ref.at[source, pl.ds(HALO, rows), :],
            dst_ref=strips_ref.at[target, pl.ds(HALO, rows), :],
            send_sem=rim_send.at[side],
            recv_sem=rim_recv.at[side],
            device_id=(lat, other),
            device_id_type=MESH,
        )

    def lat_arrived(distant, kind):
        side = far if distant else near
        target, count = ((1, strips), (strips + 1, 1), (0, 1))[kind]
        here = strips_ref.at[pl.ds(target, count), pl.ds(halo(side), HALO), :]
        pltpu.make_async_remote_copy(
            src_ref=here,
            dst_ref=here,
            send_sem=send_sem.at[distant, kind],
            recv_sem=recv_sem.at[distant, kind],
            device_id=(lat, east),
            device_id_type=MESH,
        ).wait_recv()

    for load in loads_of(0):
        load.wait()

    @pl.when(far_exists)
    def _():
        lat_copy(1, 0).start()

    for load in loads_of(1):
        load.wait()
    lat_copy(0, 0).start()
    for load in loads_of(2):
        load.wait()
    for side in range(2):
        rim_copy(side).start()
    for kind in (1, 2):
        lat_copy(0, kind).start()

    @pl.when(far_exists)
    def _():
        for kind in (1, 2):
            lat_copy(1, kind).start()

    window = Window(
        strips_ref, HALO + base, main, strips // 4, boxes, sums, coef, slope, facing, shade
    )
    lat_arrived(0, 0)

    def half(number, carry):
        @pl.when(number == 1)
        def _():
            for side in range(2):
                rim_copy(side).wait_recv()
            for kind in (1, 2):
                lat_arrived(0, kind)

        window.run(run_starts(number, strips))
        return carry

    lax.fori_loop(0, 2, half, 0)

    for pole in range(2):

        @pl.when(jnp.logical_and(jnp.logical_not(far_exists), far == pole))
        def _():
            first = HALO if pole == 0 else HALO + rows - SUB
            pick = 0 if pole == 0 else SUB - 1
            fill = 0 if pole == 0 else HALO + rows

            def repeat(strip, carry):
                row = strips_ref[strip, pl.ds(first, SUB), :][pick : pick + 1]
                block = jnp.broadcast_to(row, (SUB, LANES))
                for k in range(HALO // SUB):
                    strips_ref[strip, pl.ds(fill + k * SUB, SUB), :] = block
                return carry

            lax.fori_loop(0, strips + 2, repeat, 0)

    for side in range(2):
        rim_copy(side).wait_send()
    for kind in range(3):
        lat_copy(0, kind).wait_send()

    @pl.when(far_exists)
    def _():
        for kind in range(3):
            lat_arrived(1, kind)
            lat_copy(1, kind).wait_send()


def shade_far(rows, cols, *refs):
    strips_ref, slope, facing, shade, slope_out, facing_out, shade_out = refs[:7]
    boxes = refs[7 : 7 + SCALES]
    sums, coef, slope_far, facing_far, shade_far_, near_sem, far_sem = refs[7 + SCALES :]
    lat = lax.axis_index("lat")
    n_lat, n_lon = lax.axis_size("lat"), lax.axis_size("lon")
    far = 1 - near_side(lat)
    strips = cols // LANES
    main = rows - HALO
    base = pl.multiple_of(jnp.where(far == 0, HALO, 0), SUB)
    far_base = pl.multiple_of(jnp.where(far == 0, 0, main), SUB)
    done = [
        pltpu.make_async_copy(slope, slope_out.at[pl.ds(base, main), :], near_sem.at[0]),
        pltpu.make_async_copy(shade, shade_out.at[pl.ds(base, main), :], near_sem.at[1]),
        pltpu.make_async_copy(
            facing.at[0], facing_out.at[0, pl.ds(base, main), :], near_sem.at[2]
        ),
        pltpu.make_async_copy(
            facing.at[1], facing_out.at[1, pl.ds(base, main), :], near_sem.at[3]
        ),
    ]
    for copy in done:
        copy.start()
    fill_coef(coef, HALO, lat * rows + far_base, rows * n_lat, cols * n_lon)
    window = Window(
        strips_ref,
        HALO + far_base,
        HALO,
        strips // 4,
        boxes,
        sums,
        coef,
        slope_far,
        facing_far,
        shade_far_,
    )

    def copies(number):
        width = strips // 4 * LANES
        found = []
        for run, start in enumerate(run_starts(number, strips)):
            column = pl.ds(pl.multiple_of(start * LANES, LANES), width)
            here = pl.ds(far_base, HALO)
            for index, (source, target) in enumerate(
                (
                    (slope_far.at[:, column], slope_out.at[here, column]),
                    (shade_far_.at[:, column], shade_out.at[here, column]),
                    (facing_far.at[0, :, column], facing_out.at[0, here, column]),
                    (facing_far.at[1, :, column], facing_out.at[1, here, column]),
                )
            ):
                found.append(
                    pltpu.make_async_copy(source, target, far_sem.at[number, run, index])
                )
        return found

    def half(number, carry):
        window.run(run_starts(number, strips))
        for copy in copies(number):
            copy.start()
        return carry

    lax.fori_loop(0, 2, half, 0)
    for copy in done:
        copy.wait()
    for number in range(2):
        for copy in copies(number):
            copy.wait()


def window_scratch(count, strips):
    width = RUNS * (strips // 4)
    return [
        pltpu.VMEM((2, width, count + row_pad(k), LANES), jnp.float32) for k in range(SCALES)
    ] + [
        pltpu.VMEM((2, width, SUB, LANES), jnp.float32),
        pltpu.VMEM((count, LANES), jnp.float32),
    ]


def local(elevation):
    rows, cols = elevation.shape
    strips = cols // LANES
    main = rows - HALO
    vmem = pl.BlockSpec(memory_space=pltpu.VMEM)
    anywhere = pl.BlockSpec(memory_space=pl.ANY)
    staged = pl.pallas_call(
        functools.partial(gather, rows, cols),
        out_shape=(
            pltpu.VMEM((strips + 2, rows + 2 * HALO, LANES), jnp.float32),
            pltpu.VMEM((main, cols), jnp.float32),
            pltpu.VMEM((2, main, cols), jnp.float32),
            pltpu.VMEM((main, cols), jnp.float32),
        ),
        in_specs=[pl.BlockSpec(memory_space=pltpu.HBM)],
        out_specs=(vmem,) * 4,
        scratch_shapes=window_scratch(main, strips)
        + [
            pltpu.SemaphoreType.DMA((3, strips)),
            pltpu.SemaphoreType.DMA((2, 3)),
            pltpu.SemaphoreType.DMA((2, 3)),
            pltpu.SemaphoreType.DMA((2,)),
            pltpu.SemaphoreType.DMA((2,)),
        ],
        compiler_params=pltpu.CompilerParams(
            collective_id=0, has_side_effects=True, vmem_limit_bytes=54 * 2**20
        ),
    )(elevation)
    return tuple(
        pl.pallas_call(
            functools.partial(shade_far, rows, cols),
            out_shape=(
                jax.ShapeDtypeStruct((rows, cols), jnp.float32),
                jax.ShapeDtypeStruct((2, rows, cols), jnp.float32),
                jax.ShapeDtypeStruct((rows, cols), jnp.float32),
            ),
            in_specs=[vmem] * 4,
            out_specs=(anywhere,) * 3,
            scratch_shapes=window_scratch(HALO, strips)
            + [
                pltpu.VMEM((HALO, cols), jnp.float32),
                pltpu.VMEM((2, HALO, cols), jnp.float32),
                pltpu.VMEM((HALO, cols), jnp.float32),
                pltpu.SemaphoreType.DMA((4,)),
                pltpu.SemaphoreType.DMA((2, RUNS, 4)),
            ],
            compiler_params=pltpu.CompilerParams(vmem_limit_bytes=16 * 2**20),
        )(*staged)
    )


def solution(mesh):
    in_specs = (P("lat", "lon"),)
    out_specs = (P("lat", "lon"), P(None, "lat", "lon"), P("lat", "lon"))
    return jax.shard_map(local, mesh=mesh, in_specs=in_specs, out_specs=out_specs, check_vma=False)
```

```python
import functools
import math

import jax
import jax.numpy as jnp
from jax import lax
from jax.experimental import pallas as pl
from jax.experimental.pallas import tpu as pltpu
from jax.sharding import PartitionSpec as P

SCALES = 7
HALO = 64
LANES = 128
SUB = 8
RUNS = 2
UNROLL = 4

LIGHT_UP = math.sqrt(0.5)
MESH = pl.DeviceIdType.MESH

ANGLE = (
    1.5707962050889646,
    -0.9999801696091738,
    0.7848538132927688,
    -0.6607586188432167,
    0.5557489578459907,
    -0.42189571811945836,
    0.2501265286961767,
    -0.09607630454800326,
    0.01718536914918157,
)


def row_pad(octave):
    return max(2**octave, SUB)


def rim_hops(strips):
    lon, n_lon = lax.axis_index("lon"), lax.axis_size("lon")
    hops = [(lax.rem(lon + 1, n_lon), 0)]
    if n_lon > 2:
        hops.append((lax.rem(lon + n_lon - 1, n_lon), strips + 1))
    return hops


def east_halo(strips):
    return strips + 1 if lax.axis_size("lon") > 2 else 0


def near_side(lat):
    return 1 - lax.rem(lat, 2)


def fill_coef(coef_ref, count, first_row, total_rows, total_cols):
    for start in range(0, count, SUB):
        position = first_row + start + lax.broadcasted_iota(jnp.int32, (SUB, LANES), 0)
        spacing = jnp.sin((position.astype(jnp.float32) + 0.5) * (math.pi / total_rows)) * (
            2.0 * total_rows / total_cols
        )
        coef_ref[pl.ds(start, SUB), :] = 1.0 / (8.0 * SCALES * spacing)


class Window:
    def __init__(self, strips, rows, columns, far, coef, slope, facing, shade):
        self.strips, self.rows, self.columns = strips, rows, columns
        self.width = columns // 4
        self.coef, self.slope, self.facing, self.shade = coef, slope, facing, shade
        self.top = far == 0
        self.sign = jnp.where(self.top, 1, -1)
        self.lane = lax.broadcasted_iota(jnp.int32, (SUB, LANES), 1)

    def row(self, number):
        return pl.multiple_of(
            jnp.where(self.top, number * SUB, self.rows - SUB - number * SUB), SUB
        )

    def shift(self, octave):
        lag = 2**octave
        moved = self.sign * lag
        return pl.multiple_of(moved, SUB) if lag >= SUB else moved

    def column(self, starts, run, offset, row, shift=0):
        place = pl.ds(HALO + row + shift, SUB)
        strip = starts[run] + offset
        if offset == self.width + 1:
            strip = jnp.where(strip > self.columns, east_halo(self.columns), strip)
        return self.strips[strip, place, :]

    def near(self, starts, row):
        return [
            [self.column(starts, run, k, row) for k in range(self.width + 2)]
            for run in range(RUNS)
        ]

    def box(self, starts, row, octave, near, shift):
        lag = 2**octave
        boxes, shifted = [], []
        for run, z in enumerate(near):
            pair = []
            for k in range(self.width + 2):
                total = z[k] + self.column(starts, run, k, row, shift)
                pair.append(total * (1.0 / lag) if octave else total)
            ahead = [pltpu.roll(v, LANES - lag, 1) for v in pair]
            if 2 * lag == LANES:
                plus = [
                    jnp.where(self.lane < lag, ahead[k], ahead[k + 1])
                    for k in range(self.width + 1)
                ]
                boxes += [pair[k + 1] + plus[k + 1] for k in range(self.width)]
                shifted += [pair[k + 1] + plus[k] for k in range(self.width)]
            else:
                behind = [pltpu.roll(v, lag, 1) for v in pair]
                for k in range(1, self.width + 1):
                    plus = jnp.where(self.lane < LANES - lag, ahead[k], ahead[k + 1])
                    minus = jnp.where(self.lane >= lag, behind[k], behind[k - 1])
                    boxes.append(pair[k] + plus)
                    shifted.append(pair[k] + minus)
        return boxes, shifted

    def add(self, lags, starts, row):
        near = self.near(starts, row)
        count = RUNS * self.width
        first = second = None
        for octave in range(SCALES):
            shift = self.shift(octave)
            boxes, shifted = self.box(starts, row, octave, near, shift)
            here = row_pad(octave) + row
            for k in range(count):
                lags[octave][0, k, pl.ds(pl.multiple_of(here, SUB), SUB), :] = boxes[k]
                lags[octave][1, k, pl.ds(pl.multiple_of(here, SUB), SUB), :] = shifted[k]
            past = pl.ds(here - shift, SUB)
            u = [boxes[k] - lags[octave][1, k, past, :] for k in range(count)]
            v = [lags[octave][0, k, past, :] - shifted[k] for k in range(count)]
            first = u if first is None else [a + b for a, b in zip(first, u)]
            second = v if second is None else [a + b for a, b in zip(second, v)]
        return first, second

    def finish(self, starts, row, first, second):
        rows = pl.ds(pl.multiple_of(row, SUB), SUB)
        coef = self.coef[rows, :]
        turn = jnp.where(self.top, 1.0, -1.0) * (1.0 / (8.0 * SCALES))
        for k in range(RUNS * self.width):
            run, within = divmod(k, self.width)
            column = pl.ds(pl.multiple_of((starts[run] + within) * LANES, LANES), LANES)
            grad_east = (first[k] + second[k]) * coef
            grad_north = (second[k] - first[k]) * turn
            squared = grad_east * grad_east + grad_north * grad_north
            inverse = lax.rsqrt(1.0 + squared)
            sine = squared * lax.rsqrt(jnp.maximum(squared, 1e-37)) * inverse
            ratio = jnp.full_like(inverse, ANGLE[-1])
            for term in ANGLE[-2::-1]:
                ratio = ratio * inverse + term
            self.slope[rows, column] = sine * ratio
            self.facing[0, rows, column] = -grad_east * inverse
            self.facing[1, rows, column] = -grad_north * inverse
            tilt = 0.5 * (grad_east - grad_north) + LIGHT_UP
            self.shade[rows, column] = jnp.maximum(tilt * inverse, 0.0)


def run_starts(half, strips):
    quarter = strips // 4
    return (
        jnp.where(half == 0, quarter, 0),
        jnp.where(half == 0, 2 * quarter, 3 * quarter),
    )


def gather(rows, cols, z_ref, strips_ref, part, slope, facing, shade, *scratch):
    lags, (rim, coef, load_sem, send_sem, recv_sem, rim_send, rim_recv) = (
        scratch[:SCALES],
        scratch[SCALES:],
    )
    lat, lon = lax.axis_index("lat"), lax.axis_index("lon")
    n_lat, n_lon = lax.axis_size("lat"), lax.axis_size("lon")
    strips = cols // LANES
    hops = rim_hops(strips)
    width = strips // 4
    count = RUNS * width
    near = near_side(lat)
    far = 1 - near
    exists = (lat > 0, lat < n_lat - 1)
    far_exists = jnp.where(far == 0, exists[0], exists[1])
    far_lat = jnp.where(far == 0, lat - 1, lat + 1)
    near_lat = jnp.where(near == 0, lat - 1, lat + 1)

    def edge(side):
        return pl.multiple_of(jnp.where(side == 0, 0, rows - HALO), SUB)

    def halo(side):
        return pl.multiple_of(jnp.where(side == 0, 0, HALO + rows), SUB)

    def loads_of(number):
        start, size = ((edge(far), HALO), (edge(near), HALO), (HALO, rows - 2 * HALO))[number]
        return [
            pltpu.make_async_copy(
                z_ref.at[pl.ds(start, size), pl.ds(strip * LANES, LANES)],
                strips_ref.at[1 + strip, pl.ds(HALO + start, size), :],
                load_sem.at[number, strip],
            )
            for strip in range(strips)
        ]

    for number in range(3):
        for load in loads_of(number):
            load.start()

    barrier = pltpu.get_barrier_semaphore()

    @pl.when(far_exists)
    def _():
        for other in [lon] + [hop for hop, _ in hops]:
            pl.semaphore_signal(barrier, inc=1, device_id=(far_lat, other), device_id_type=MESH)

    for other, _ in hops:
        pl.semaphore_signal(barrier, inc=1, device_id=(lat, other), device_id_type=MESH)
    for other in [lon] + [hop for hop, _ in hops]:
        pl.semaphore_signal(barrier, inc=1, device_id=(near_lat, other), device_id_type=MESH)

    main = rows - HALO
    base = pl.multiple_of(jnp.where(far == 0, HALO, 0), SUB)
    fill_coef(coef, main, lat * rows + base, rows * n_lat, cols * n_lon)
    for load in loads_of(0):
        load.wait()
    greeted = 1 + len(hops)
    pl.semaphore_wait(barrier, greeted + len(hops) + greeted * far_exists.astype(jnp.int32))

    def lat_copy(distant):
        side, other = (far, far_lat) if distant else (near, near_lat)
        return pltpu.make_async_remote_copy(
            src_ref=strips_ref.at[pl.ds(1, strips), pl.ds(HALO + edge(side), HALO), :],
            dst_ref=strips_ref.at[pl.ds(1, strips), pl.ds(halo(1 - side), HALO), :],
            send_sem=send_sem.at[distant, 0],
            recv_sem=recv_sem.at[distant, 0],
            device_id=(other, lon),
            device_id_type=MESH,
        )

    def corner_copy(distant, index):
        side, other = (far, far_lat) if distant else (near, near_lat)
        hop, target = hops[index]
        return pltpu.make_async_remote_copy(
            src_ref=rim.at[pl.ds(edge(side), HALO), :],
            dst_ref=strips_ref.at[target, pl.ds(halo(1 - side), HALO), :],
            send_sem=send_sem.at[distant, 1 + index],
            recv_sem=recv_sem.at[distant, 1 + index],
            device_id=(other, hop),
            device_id_type=MESH,
        )

    def rim_copy(index):
        hop, target = hops[index]
        return pltpu.make_async_remote_copy(
            src_ref=rim,
            dst_ref=strips_ref.at[target, pl.ds(HALO, rows), :],
            send_sem=rim_send.at[index],
            recv_sem=rim_recv.at[index],
            device_id=(lat, hop),
            device_id_type=MESH,
        )

    def arrived(distant, kind):
        here = pl.ds(halo(far if distant else near), HALO)
        if kind == 0:
            place = strips_ref.at[pl.ds(1, strips), here, :]
        else:
            place = strips_ref.at[hops[kind - 1][1], here, :]
        pltpu.make_async_remote_copy(
            src_ref=place,
            dst_ref=place,
            send_sem=send_sem.at[distant, kind],
            recv_sem=recv_sem.at[distant, kind],
            device_id=(lat, hops[0][0]),
            device_id_type=MESH,
        ).wait_recv()

    @pl.when(far_exists)
    def _():
        lat_copy(1).start()

    for load in loads_of(1):
        load.wait()
    lat_copy(0).start()
    for load in loads_of(2):
        load.wait()
    lane = lax.broadcasted_iota(jnp.int32, (SUB, LANES), 1)
    for start in range(0, rows, SUB):
        here = pl.ds(HALO + start, SUB)
        rim[pl.ds(start, SUB), :] = jnp.where(
            lane < HALO, strips_ref[1, here, :], strips_ref[strips, here, :]
        )

    for octave in range(SCALES):
        pad = row_pad(octave)
        first = pl.multiple_of(jnp.where(far == 0, 0, pad + rows), SUB)
        for k in range(count):
            for start in range(0, pad, SUB):
                for which in range(2):
                    lags[octave][which, k, pl.ds(first + start, SUB), :] = jnp.zeros(
                        (SUB, LANES), jnp.float32
                    )

    for index in range(len(hops)):
        rim_copy(index).start()
        corner_copy(0, index).start()

    @pl.when(far_exists)
    def _():
        for index in range(len(hops)):
            corner_copy(1, index).start()

    window = Window(strips_ref, rows, strips, far, coef, slope, facing, shade)
    far_base = pl.multiple_of(jnp.where(far == 0, 0, main), SUB)

    def half(number, carry):
        @pl.when(number == 1)
        def _():
            for index in range(len(hops)):
                rim_copy(index).wait_recv()
                arrived(0, 1 + index)

        starts = run_starts(number, strips)

        def partly(block, carry):
            for inner in range(UNROLL):
                row = window.row(block * UNROLL + inner)
                found = window.add(lags, starts, row)
                rows_here = pl.ds(pl.multiple_of(row - far_base, SUB), SUB)
                for which in range(2):
                    for k in range(count):
                        run, within = divmod(k, width)
                        part[which, starts[run] + within, rows_here, :] = found[which][k]
            return carry

        def fully(block, carry):
            for inner in range(UNROLL):
                row = window.row(block * UNROLL + inner)
                window.finish(starts, row - base, *window.add(lags, starts, row))
            return carry

        size = UNROLL * SUB
        lax.fori_loop(0, HALO // size, partly, 0)
        lax.fori_loop(HALO // size, (rows - HALO) // size, fully, 0)

        @pl.when(number == 0)
        def _():
            arrived(0, 0)

        lax.fori_loop((rows - HALO) // size, rows // size, fully, 0)
        return carry

    lax.fori_loop(0, 2, half, 0)

    for pole in range(2):

        @pl.when(jnp.logical_and(jnp.logical_not(far_exists), far == pole))
        def _():
            first = HALO if pole == 0 else HALO + rows - SUB
            pick = 0 if pole == 0 else SUB - 1
            fill = 0 if pole == 0 else HALO + rows

            def repeat(strip, carry):
                row = strips_ref[strip, pl.ds(first, SUB), :][pick : pick + 1]
                block = jnp.broadcast_to(row, (SUB, LANES))
                for k in range(HALO // SUB):
                    strips_ref[strip, pl.ds(fill + k * SUB, SUB), :] = block
                return carry

            lax.fori_loop(0, strips_ref.shape[0], repeat, 0)

    lat_copy(0).wait_send()
    for index in range(len(hops)):
        rim_copy(index).wait_send()
        corner_copy(0, index).wait_send()

    @pl.when(far_exists)
    def _():
        lat_copy(1).wait_send()
        arrived(1, 0)
        for index in range(len(hops)):
            corner_copy(1, index).wait_send()
            arrived(1, 1 + index)


def shade_far(rows, cols, *refs):
    strips_ref, part, slope, facing, shade, slope_out, facing_out, shade_out = refs[:8]
    coef, slope_far, facing_far, shade_far_, near_sem, far_sem = refs[8:]
    lat = lax.axis_index("lat")
    n_lat, n_lon = lax.axis_size("lat"), lax.axis_size("lon")
    far = 1 - near_side(lat)
    strips = cols // LANES
    width = strips // 4
    count = RUNS * width
    main = rows - HALO
    base = pl.multiple_of(jnp.where(far == 0, HALO, 0), SUB)
    far_base = pl.multiple_of(jnp.where(far == 0, 0, main), SUB)
    done = [
        pltpu.make_async_copy(source, target, near_sem.at[index])
        for index, (source, target) in enumerate(
            (
                (slope, slope_out.at[pl.ds(base, main), :]),
                (shade, shade_out.at[pl.ds(base, main), :]),
                (facing.at[0], facing_out.at[0, pl.ds(base, main), :]),
                (facing.at[1], facing_out.at[1, pl.ds(base, main), :]),
            )
        )
    ]
    for copy in done:
        copy.start()
    fill_coef(coef, HALO, lat * rows + far_base, rows * n_lat, cols * n_lon)
    window = Window(strips_ref, rows, strips, far, coef, slope_far, facing_far, shade_far_)
    sublane = lax.broadcasted_iota(jnp.int32, (SUB, LANES), 0)

    def copies(number):
        found = []
        for run, start in enumerate(run_starts(number, strips)):
            column = pl.ds(pl.multiple_of(start * LANES, LANES), width * LANES)
            here = pl.ds(far_base, HALO)
            for index, (source, target) in enumerate(
                (
                    (slope_far.at[:, column], slope_out.at[here, column]),
                    (shade_far_.at[:, column], shade_out.at[here, column]),
                    (facing_far.at[0, :, column], facing_out.at[0, here, column]),
                    (facing_far.at[1, :, column], facing_out.at[1, here, column]),
                )
            ):
                found.append(
                    pltpu.make_async_copy(source, target, far_sem.at[number, run, index])
                )
        return found

    def half(number, carry):
        starts = run_starts(number, strips)
        for step in range(HALO // SUB):
            row = window.row(step)
            local_row = pl.multiple_of(row - far_base, SUB)
            first, second = [
                [
                    part[which, starts[k // width] + k % width, pl.ds(local_row, SUB), :]
                    for k in range(count)
                ]
                for which in range(2)
            ]
            near = window.near(starts, row)
            for octave in range(SCALES):
                lag = 2**octave
                if row_pad(octave) <= step * SUB:
                    continue
                boxes, shifted = window.box(starts, row, octave, near, -window.shift(octave))
                if lag < SUB:
                    beyond = jnp.logical_or(
                        jnp.logical_and(far == 0, sublane < lag),
                        jnp.logical_and(far == 1, sublane >= SUB - lag),
                    )
                    boxes = [jnp.where(beyond, v, 0.0) for v in boxes]
                    shifted = [jnp.where(beyond, v, 0.0) for v in shifted]
                first = [a - b for a, b in zip(first, shifted)]
                second = [a + b for a, b in zip(second, boxes)]
            window.finish(starts, local_row, first, second)
        for copy in copies(number):
            copy.start()
        return carry

    lax.fori_loop(0, 2, half, 0)
    for copy in done:
        copy.wait()
    for number in range(2):
        for copy in copies(number):
            copy.wait()


def local(elevation):
    rows, cols = elevation.shape
    strips = cols // LANES
    count = RUNS * (strips // 4)
    hops = 1 if lax.axis_size("lon") == 2 else 2
    main = rows - HALO
    vmem = pl.BlockSpec(memory_space=pltpu.VMEM)
    anywhere = pl.BlockSpec(memory_space=pl.ANY)
    staged = pl.pallas_call(
        functools.partial(gather, rows, cols),
        out_shape=(
            pltpu.VMEM((strips + hops, rows + 2 * HALO, LANES), jnp.float32),
            pltpu.VMEM((2, strips, HALO, LANES), jnp.float32),
            pltpu.VMEM((main, cols), jnp.float32),
            pltpu.VMEM((2, main, cols), jnp.float32),
            pltpu.VMEM((main, cols), jnp.float32),
        ),
        in_specs=[anywhere],
        out_specs=(vmem,) * 5,
        scratch_shapes=[
            pltpu.VMEM((2, count, rows + 2 * row_pad(k), LANES), jnp.float32)
            for k in range(SCALES)
        ]
        + [
            pltpu.VMEM((rows, LANES), jnp.float32),
            pltpu.VMEM((main, LANES), jnp.float32),
            pltpu.SemaphoreType.DMA((3, strips)),
            pltpu.SemaphoreType.DMA((2, 1 + hops)),
            pltpu.SemaphoreType.DMA((2, 1 + hops)),
            pltpu.SemaphoreType.DMA((hops,)),
            pltpu.SemaphoreType.DMA((hops,)),
        ],
        compiler_params=pltpu.CompilerParams(
            collective_id=0, has_side_effects=True, vmem_limit_bytes=52 * 2**20
        ),
    )(elevation)
    return tuple(
        pl.pallas_call(
            functools.partial(shade_far, rows, cols),
            out_shape=(
                jax.ShapeDtypeStruct((rows, cols), jnp.float32),
                jax.ShapeDtypeStruct((2, rows, cols), jnp.float32),
                jax.ShapeDtypeStruct((rows, cols), jnp.float32),
            ),
            in_specs=[vmem] * 5,
            out_specs=(anywhere,) * 3,
            scratch_shapes=[
                pltpu.VMEM((HALO, LANES), jnp.float32),
                pltpu.VMEM((HALO, cols), jnp.float32),
                pltpu.VMEM((2, HALO, cols), jnp.float32),
                pltpu.VMEM((HALO, cols), jnp.float32),
                pltpu.SemaphoreType.DMA((4,)),
                pltpu.SemaphoreType.DMA((2, RUNS, 4)),
            ],
            compiler_params=pltpu.CompilerParams(vmem_limit_bytes=16 * 2**20),
        )(*staged)
    )


def solution(mesh):
    in_specs = (P("lat", "lon"),)
    out_specs = (P("lat", "lon"), P(None, "lat", "lon"), P("lat", "lon"))
    return jax.shard_map(local, mesh=mesh, in_specs=in_specs, out_specs=out_specs, check_vma=False)
```

```python
import functools
import math

import jax
import jax.numpy as jnp
from jax import lax
from jax.experimental import pallas as pl
from jax.experimental.pallas import tpu as pltpu
from jax.sharding import PartitionSpec as P

SCALES = 7
HALO = 64
LANES = 128
SUB = 8
RUNS = 2
UNROLL = 4

LIGHT_UP = math.sqrt(0.5)
MESH = pl.DeviceIdType.MESH

ANGLE = (
    1.5707962050889646,
    -0.9999801696091738,
    0.7848538132927688,
    -0.6607586188432167,
    0.5557489578459907,
    -0.42189571811945836,
    0.2501265286961767,
    -0.09607630454800326,
    0.01718536914918157,
)


def spread(rows):
    return rows + (-rows // SUB + 1) % 4 * SUB


def row_pad(octave):
    return max(2**octave, SUB)


def rim_hops(strips):
    lon, n_lon = lax.axis_index("lon"), lax.axis_size("lon")
    hops = [(lax.rem(lon + 1, n_lon), 0)]
    if n_lon > 2:
        hops.append((lax.rem(lon + n_lon - 1, n_lon), strips + 1))
    return hops


def east_halo(strips):
    return strips + 1 if lax.axis_size("lon") > 2 else 0


def near_side(lat):
    return 1 - lax.rem(lat, 2)


def fill_coef(coef_ref, count, first_row, total_rows, total_cols):
    for start in range(0, count, SUB):
        position = first_row + start + lax.broadcasted_iota(jnp.int32, (SUB, LANES), 0)
        spacing = jnp.sin((position.astype(jnp.float32) + 0.5) * (math.pi / total_rows)) * (
            2.0 * total_rows / total_cols
        )
        coef_ref[pl.ds(start, SUB), :] = 1.0 / (8.0 * SCALES * spacing)


class Window:
    def __init__(self, strips, rows, columns, far, coef, slope, facing, shade):
        self.strips, self.rows, self.columns = strips, rows, columns
        self.width = columns // 4
        self.coef, self.slope, self.facing, self.shade = coef, slope, facing, shade
        self.top = far == 0
        self.sign = jnp.where(self.top, 1, -1)
        self.lane = lax.broadcasted_iota(jnp.int32, (SUB, LANES), 1)

    def row(self, number):
        return pl.multiple_of(
            jnp.where(self.top, number * SUB, self.rows - SUB - number * SUB), SUB
        )

    def shift(self, octave):
        lag = 2**octave
        moved = self.sign * lag
        return pl.multiple_of(moved, SUB) if lag >= SUB else moved

    def column(self, starts, run, offset, row, shift=0):
        place = pl.ds(HALO + row + shift, SUB)
        strip = starts[run] + offset
        if offset == self.width + 1:
            strip = jnp.where(strip > self.columns, east_halo(self.columns), strip)
        return self.strips[strip, place, :]

    def near(self, starts, row, runs):
        return [
            (run, [self.column(starts, run, k, row) for k in range(self.width + 2)])
            for run in runs
        ]

    def box(self, starts, row, octave, near, shift):
        lag = 2**octave
        boxes, shifted = [], []
        for run, z in near:
            pair = []
            for k in range(self.width + 2):
                total = z[k] + self.column(starts, run, k, row, shift)
                pair.append(total * (1.0 / lag) if octave else total)
            ahead = [pltpu.roll(v, LANES - lag, 1) for v in pair]
            if 2 * lag == LANES:
                plus = [
                    jnp.where(self.lane < lag, ahead[k], ahead[k + 1])
                    for k in range(self.width + 1)
                ]
                boxes += [pair[k + 1] + plus[k + 1] for k in range(self.width)]
                shifted += [pair[k + 1] + plus[k] for k in range(self.width)]
            else:
                behind = [pltpu.roll(v, lag, 1) for v in pair]
                for k in range(1, self.width + 1):
                    plus = jnp.where(self.lane < LANES - lag, ahead[k], ahead[k + 1])
                    minus = jnp.where(self.lane >= lag, behind[k], behind[k - 1])
                    boxes.append(pair[k] + plus)
                    shifted.append(pair[k] + minus)
        return boxes, shifted

    def add(self, lags, starts, row, run):
        near = self.near(starts, row, [run])
        count = self.width
        low = run * self.width
        first = second = None
        for octave in range(SCALES):
            shift = self.shift(octave)
            boxes, shifted = self.box(starts, row, octave, near, shift)
            here = row_pad(octave) + row
            for k in range(count):
                lags[octave][0, low + k, pl.ds(pl.multiple_of(here, SUB), SUB), :] = boxes[k]
                lags[octave][1, low + k, pl.ds(pl.multiple_of(here, SUB), SUB), :] = shifted[k]
            past = pl.ds(here - shift, SUB)
            u = [boxes[k] - lags[octave][1, low + k, past, :] for k in range(count)]
            v = [lags[octave][0, low + k, past, :] - shifted[k] for k in range(count)]
            first = u if first is None else [a + b for a, b in zip(first, u)]
            second = v if second is None else [a + b for a, b in zip(second, v)]
        return first, second

    def finish(self, starts, row, first, second, runs=(0, 1)):
        rows = pl.ds(pl.multiple_of(row, SUB), SUB)
        coef = self.coef[rows, :]
        turn = jnp.where(self.top, 1.0, -1.0) * (1.0 / (8.0 * SCALES))
        for k in range(len(runs) * self.width):
            run, within = runs[k // self.width], k % self.width
            column = pl.ds(pl.multiple_of((starts[run] + within) * LANES, LANES), LANES)
            grad_east = (first[k] + second[k]) * coef
            grad_north = (second[k] - first[k]) * turn
            squared = grad_east * grad_east + grad_north * grad_north
            inverse = lax.rsqrt(1.0 + squared)
            sine = squared * lax.rsqrt(jnp.maximum(squared, 1e-37)) * inverse
            ratio = jnp.full_like(inverse, ANGLE[-1])
            for term in ANGLE[-2::-1]:
                ratio = ratio * inverse + term
            self.slope[rows, column] = sine * ratio
            turned = -inverse
            self.facing[0, rows, column] = grad_east * turned
            self.facing[1, rows, column] = grad_north * turned
            tilt = 0.5 * (grad_east - grad_north) + LIGHT_UP
            self.shade[rows, column] = jnp.maximum(tilt * inverse, 0.0)


def run_starts(half, strips):
    quarter = strips // 4
    return (
        jnp.where(half == 0, quarter, 0),
        jnp.where(half == 0, 2 * quarter, 3 * quarter),
    )


def gather(rows, cols, z_ref, strips_ref, part, slope, facing, shade, *scratch):
    lags, (rim, coef, greeted, load_sem, send_sem, recv_sem, rim_send, rim_recv) = (
        scratch[:SCALES],
        scratch[SCALES:],
    )
    lat, lon = lax.axis_index("lat"), lax.axis_index("lon")
    n_lat, n_lon = lax.axis_size("lat"), lax.axis_size("lon")
    strips = cols // LANES
    hops = rim_hops(strips)
    width = strips // 4
    count = RUNS * width
    near = near_side(lat)
    far = 1 - near
    exists = (lat > 0, lat < n_lat - 1)
    far_exists = jnp.where(far == 0, exists[0], exists[1])
    far_lat = jnp.where(far == 0, lat - 1, lat + 1)
    near_lat = jnp.where(near == 0, lat - 1, lat + 1)

    def edge(side):
        return pl.multiple_of(jnp.where(side == 0, 0, rows - HALO), SUB)

    def halo(side):
        return pl.multiple_of(jnp.where(side == 0, 0, HALO + rows), SUB)

    def loads_of(number):
        start, size = ((edge(far), HALO), (edge(near), HALO), (HALO, rows - 2 * HALO))[number]
        return [
            pltpu.make_async_copy(
                z_ref.at[pl.ds(start, size), pl.ds(strip * LANES, LANES)],
                strips_ref.at[1 + strip, pl.ds(HALO + start, size), :],
                load_sem.at[number, strip],
            )
            for strip in range(strips)
        ]

    for number in range(3):
        for load in loads_of(number):
            load.start()

    barrier = pltpu.get_barrier_semaphore()

    @pl.when(far_exists)
    def _():
        pl.semaphore_signal(barrier, inc=1, device_id=(far_lat, lon), device_id_type=MESH)

    for hop, _ in hops:
        pl.semaphore_signal(barrier, inc=1, device_id=(lat, hop), device_id_type=MESH)
    pl.semaphore_signal(barrier, inc=1, device_id=(near_lat, lon), device_id_type=MESH)

    main = rows - HALO
    base = pl.multiple_of(jnp.where(far == 0, HALO, 0), SUB)
    fill_coef(coef, main, lat * rows + base, rows * n_lat, cols * n_lon)
    for load in loads_of(0):
        load.wait()
    pl.semaphore_wait(barrier, 1 + len(hops) + far_exists.astype(jnp.int32))
    for hop, _ in hops:
        pl.semaphore_signal(greeted, inc=1, device_id=(lat, hop), device_id_type=MESH)

    def lat_copy(distant):
        side, other = (far, far_lat) if distant else (near, near_lat)
        return pltpu.make_async_remote_copy(
            src_ref=strips_ref.at[pl.ds(1, strips), pl.ds(HALO + edge(side), HALO), :],
            dst_ref=strips_ref.at[pl.ds(1, strips), pl.ds(halo(1 - side), HALO), :],
            send_sem=send_sem.at[distant, 0],
            recv_sem=recv_sem.at[distant, 0],
            device_id=(other, lon),
            device_id_type=MESH,
        )

    def corner_copy(distant, index):
        side, other = (far, far_lat) if distant else (near, near_lat)
        hop, target = hops[index]
        return pltpu.make_async_remote_copy(
            src_ref=rim.at[pl.ds(edge(side), HALO), :],
            dst_ref=strips_ref.at[target, pl.ds(halo(1 - side), HALO), :],
            send_sem=send_sem.at[distant, 1 + index],
            recv_sem=recv_sem.at[distant, 1 + index],
            device_id=(other, hop),
            device_id_type=MESH,
        )

    def rim_copy(index):
        hop, target = hops[index]
        return pltpu.make_async_remote_copy(
            src_ref=rim,
            dst_ref=strips_ref.at[target, pl.ds(HALO, rows), :],
            send_sem=rim_send.at[index],
            recv_sem=rim_recv.at[index],
            device_id=(lat, hop),
            device_id_type=MESH,
        )

    def arrived(distant, kind):
        here = pl.ds(halo(far if distant else near), HALO)
        if kind == 0:
            place = strips_ref.at[pl.ds(1, strips), here, :]
        else:
            place = strips_ref.at[hops[kind - 1][1], here, :]
        pltpu.make_async_remote_copy(
            src_ref=place,
            dst_ref=place,
            send_sem=send_sem.at[distant, kind],
            recv_sem=recv_sem.at[distant, kind],
            device_id=(lat, hops[0][0]),
            device_id_type=MESH,
        ).wait_recv()

    @pl.when(far_exists)
    def _():
        lat_copy(1).start()

    for load in loads_of(1):
        load.wait()
    lat_copy(0).start()
    for load in loads_of(2):
        load.wait()
    lane = lax.broadcasted_iota(jnp.int32, (SUB, LANES), 1)
    for start in range(0, rows, SUB):
        here = pl.ds(HALO + start, SUB)
        rim[pl.ds(start, SUB), :] = jnp.where(
            lane < HALO, strips_ref[1, here, :], strips_ref[strips, here, :]
        )

    for octave in range(SCALES):
        pad = row_pad(octave)
        first = pl.multiple_of(jnp.where(far == 0, 0, pad + rows), SUB)
        for k in range(count):
            for start in range(0, pad, SUB):
                for which in range(2):
                    lags[octave][which, k, pl.ds(first + start, SUB), :] = jnp.zeros(
                        (SUB, LANES), jnp.float32
                    )

    for index in range(len(hops)):
        rim_copy(index).start()
    pl.semaphore_wait(greeted, len(hops))
    for index in range(len(hops)):
        corner_copy(0, index).start()

    @pl.when(far_exists)
    def _():
        for index in range(len(hops)):
            corner_copy(1, index).start()

    window = Window(strips_ref, rows, strips, far, coef, slope, facing, shade)
    far_base = pl.multiple_of(jnp.where(far == 0, 0, main), SUB)

    def half(number, carry):
        @pl.when(number == 1)
        def _():
            for index in range(len(hops)):
                rim_copy(index).wait_recv()
                arrived(0, 1 + index)

        starts = run_starts(number, strips)

        def partly(block, carry):
            for inner in range(UNROLL):
                row = window.row(block * UNROLL + inner)
                rows_here = pl.ds(pl.multiple_of(row - far_base, SUB), SUB)
                for run in range(RUNS):
                    found = window.add(lags, starts, row, run)
                    for which in range(2):
                        for k in range(width):
                            part[which, starts[run] + k, rows_here, :] = found[which][k]
            return carry

        def fully(block, carry):
            for inner in range(UNROLL):
                row = window.row(block * UNROLL + inner)
                for run in range(RUNS):
                    window.finish(
                        starts, row - base, *window.add(lags, starts, row, run), runs=(run,)
                    )
            return carry

        size = UNROLL * SUB
        lax.fori_loop(0, HALO // size, partly, 0)

        @pl.when(number == 0)
        def _():
            arrived(0, 0)

        lax.fori_loop(HALO // size, rows // size, fully, 0)
        return carry

    lax.fori_loop(0, 2, half, 0)

    for pole in range(2):

        @pl.when(jnp.logical_and(jnp.logical_not(far_exists), far == pole))
        def _():
            first = HALO if pole == 0 else HALO + rows - SUB
            pick = 0 if pole == 0 else SUB - 1
            fill = 0 if pole == 0 else HALO + rows

            def repeat(strip, carry):
                row = strips_ref[strip, pl.ds(first, SUB), :][pick : pick + 1]
                block = jnp.broadcast_to(row, (SUB, LANES))
                for k in range(HALO // SUB):
                    strips_ref[strip, pl.ds(fill + k * SUB, SUB), :] = block
                return carry

            lax.fori_loop(0, strips_ref.shape[0], repeat, 0)

    lat_copy(0).wait_send()
    for index in range(len(hops)):
        rim_copy(index).wait_send()
        corner_copy(0, index).wait_send()

    @pl.when(far_exists)
    def _():
        lat_copy(1).wait_send()
        arrived(1, 0)
        for index in range(len(hops)):
            corner_copy(1, index).wait_send()
            arrived(1, 1 + index)


def shade_far(rows, cols, *refs):
    strips_ref, part, slope, facing, shade, slope_out, facing_out, shade_out = refs[:8]
    coef, slope_far, facing_far, shade_far_, near_sem, far_sem = refs[8:]
    lat = lax.axis_index("lat")
    n_lat, n_lon = lax.axis_size("lat"), lax.axis_size("lon")
    far = 1 - near_side(lat)
    strips = cols // LANES
    width = strips // 4
    count = RUNS * width
    main = rows - HALO
    base = pl.multiple_of(jnp.where(far == 0, HALO, 0), SUB)
    far_base = pl.multiple_of(jnp.where(far == 0, 0, main), SUB)
    done = [
        pltpu.make_async_copy(source, target, near_sem.at[index])
        for index, (source, target) in enumerate(
            (
                (slope, slope_out.at[pl.ds(base, main), :]),
                (shade, shade_out.at[pl.ds(base, main), :]),
                (facing.at[0], facing_out.at[0, pl.ds(base, main), :]),
                (facing.at[1], facing_out.at[1, pl.ds(base, main), :]),
            )
        )
    ]
    for copy in done:
        copy.start()
    fill_coef(coef, HALO, lat * rows + far_base, rows * n_lat, cols * n_lon)
    window = Window(strips_ref, rows, strips, far, coef, slope_far, facing_far, shade_far_)
    sublane = lax.broadcasted_iota(jnp.int32, (SUB, LANES), 0)

    def copies(number):
        found = []
        for run, start in enumerate(run_starts(number, strips)):
            column = pl.ds(pl.multiple_of(start * LANES, LANES), width * LANES)
            here = pl.ds(far_base, HALO)
            for index, (source, target) in enumerate(
                (
                    (slope_far.at[:, column], slope_out.at[here, column]),
                    (shade_far_.at[:, column], shade_out.at[here, column]),
                    (facing_far.at[0, :, column], facing_out.at[0, here, column]),
                    (facing_far.at[1, :, column], facing_out.at[1, here, column]),
                )
            ):
                found.append(
                    pltpu.make_async_copy(source, target, far_sem.at[number, run, index])
                )
        return found

    def half(number, carry):
        starts = run_starts(number, strips)
        for step in range(HALO // SUB):
            row = window.row(step)
            local_row = pl.multiple_of(row - far_base, SUB)
            first, second = [
                [
                    part[which, starts[k // width] + k % width, pl.ds(local_row, SUB), :]
                    for k in range(count)
                ]
                for which in range(2)
            ]
            near = window.near(starts, row, range(RUNS))
            for octave in range(SCALES):
                lag = 2**octave
                if row_pad(octave) <= step * SUB:
                    continue
                boxes, shifted = window.box(starts, row, octave, near, -window.shift(octave))
                if lag < SUB:
                    beyond = jnp.logical_or(
                        jnp.logical_and(far == 0, sublane < lag),
                        jnp.logical_and(far == 1, sublane >= SUB - lag),
                    )
                    boxes = [jnp.where(beyond, v, 0.0) for v in boxes]
                    shifted = [jnp.where(beyond, v, 0.0) for v in shifted]
                first = [a - b for a, b in zip(first, shifted)]
                second = [a + b for a, b in zip(second, boxes)]
            window.finish(starts, local_row, first, second)
        for copy in copies(number):
            copy.start()
        return carry

    lax.fori_loop(0, 2, half, 0)
    for copy in done:
        copy.wait()
    for number in range(2):
        for copy in copies(number):
            copy.wait()


def local(elevation):
    rows, cols = elevation.shape
    strips = cols // LANES
    count = RUNS * (strips // 4)
    hops = 1 if lax.axis_size("lon") == 2 else 2
    main = rows - HALO
    vmem = pl.BlockSpec(memory_space=pltpu.VMEM)
    anywhere = pl.BlockSpec(memory_space=pl.ANY)
    staged = pl.pallas_call(
        functools.partial(gather, rows, cols),
        out_shape=(
            pltpu.VMEM((strips + hops, spread(rows + 2 * HALO), LANES), jnp.float32),
            pltpu.VMEM((2, strips, HALO, LANES), jnp.float32),
            pltpu.VMEM((main, cols), jnp.float32),
            pltpu.VMEM((2, main, cols), jnp.float32),
            pltpu.VMEM((main, cols), jnp.float32),
        ),
        in_specs=[anywhere],
        out_specs=(vmem,) * 5,
        scratch_shapes=[
            pltpu.VMEM((2, count, spread(rows + 2 * row_pad(k)), LANES), jnp.float32)
            for k in range(SCALES)
        ]
        + [
            pltpu.VMEM((rows, LANES), jnp.float32),
            pltpu.VMEM((main, LANES), jnp.float32),
            pltpu.SemaphoreType.REGULAR,
            pltpu.SemaphoreType.DMA((3, strips)),
            pltpu.SemaphoreType.DMA((2, 1 + hops)),
            pltpu.SemaphoreType.DMA((2, 1 + hops)),
            pltpu.SemaphoreType.DMA((hops,)),
            pltpu.SemaphoreType.DMA((hops,)),
        ],
        compiler_params=pltpu.CompilerParams(
            collective_id=0, has_side_effects=True, vmem_limit_bytes=52 * 2**20
        ),
    )(elevation)
    return tuple(
        pl.pallas_call(
            functools.partial(shade_far, rows, cols),
            out_shape=(
                jax.ShapeDtypeStruct((rows, cols), jnp.float32),
                jax.ShapeDtypeStruct((2, rows, cols), jnp.float32),
                jax.ShapeDtypeStruct((rows, cols), jnp.float32),
            ),
            in_specs=[vmem] * 5,
            out_specs=(anywhere,) * 3,
            scratch_shapes=[
                pltpu.VMEM((HALO, LANES), jnp.float32),
                pltpu.VMEM((HALO, cols), jnp.float32),
                pltpu.VMEM((2, HALO, cols), jnp.float32),
                pltpu.VMEM((HALO, cols), jnp.float32),
                pltpu.SemaphoreType.DMA((4,)),
                pltpu.SemaphoreType.DMA((2, RUNS, 4)),
            ],
            compiler_params=pltpu.CompilerParams(vmem_limit_bytes=16 * 2**20),
        )(*staged)
    )


def solution(mesh):
    in_specs = (P("lat", "lon"),)
    out_specs = (P("lat", "lon"), P(None, "lat", "lon"), P("lat", "lon"))
    return jax.shard_map(local, mesh=mesh, in_specs=in_specs, out_specs=out_specs, check_vma=False)
```

```python
import functools
import math

import jax
import jax.numpy as jnp
from jax import lax
from jax.experimental import pallas as pl
from jax.experimental.pallas import tpu as pltpu
from jax.sharding import PartitionSpec as P

SCALES = 7
HALO = 64
LANES = 128
SUB = 8
RUNS = 2
UNROLL = 4

LIGHT_UP = math.sqrt(0.5)
MESH = pl.DeviceIdType.MESH

ANGLE = (
    1.5707962050889646,
    -0.9999801696091738,
    0.7848538132927688,
    -0.6607586188432167,
    0.5557489578459907,
    -0.42189571811945836,
    0.2501265286961767,
    -0.09607630454800326,
    0.01718536914918157,
)


def spread(rows):
    return rows + (-rows // SUB + 1) % 4 * SUB


def row_pad(octave):
    return max(2**octave, SUB)


def rim_hops(strips):
    lon, n_lon = lax.axis_index("lon"), lax.axis_size("lon")
    hops = [(lax.rem(lon + 1, n_lon), 0)]
    if n_lon > 2:
        hops.append((lax.rem(lon + n_lon - 1, n_lon), strips + 1))
    return hops


def east_halo(strips):
    return strips + 1 if lax.axis_size("lon") > 2 else 0


def near_side(lat):
    return 1 - lax.rem(lat, 2)


def fill_coef(coef_ref, count, first_row, total_rows, total_cols):
    for start in range(0, count, SUB):
        position = first_row + start + lax.broadcasted_iota(jnp.int32, (SUB, LANES), 0)
        spacing = jnp.sin((position.astype(jnp.float32) + 0.5) * (math.pi / total_rows)) * (
            2.0 * total_rows / total_cols
        )
        coef_ref[pl.ds(start, SUB), :] = 1.0 / (8.0 * SCALES * spacing)


class Window:
    def __init__(self, strips, rows, columns, far, coef, slope, facing, shade):
        self.strips, self.rows, self.columns = strips, rows, columns
        self.width = columns // 4
        self.coef, self.slope, self.facing, self.shade = coef, slope, facing, shade
        self.top = far == 0
        self.sign = jnp.where(self.top, 1, -1)
        self.lane = lax.broadcasted_iota(jnp.int32, (SUB, LANES), 1)

    def row(self, number):
        return pl.multiple_of(
            jnp.where(self.top, number * SUB, self.rows - SUB - number * SUB), SUB
        )

    def shift(self, octave):
        lag = 2**octave
        moved = self.sign * lag
        return pl.multiple_of(moved, SUB) if lag >= SUB else moved

    def column(self, starts, run, offset, row, shift=0):
        place = pl.ds(HALO + row + shift, SUB)
        strip = starts[run] + offset
        if offset == self.width + 1:
            strip = jnp.where(strip > self.columns, east_halo(self.columns), strip)
        return self.strips[strip, place, :]

    def near(self, starts, row, runs):
        return [
            (run, [self.column(starts, run, k, row) for k in range(self.width + 2)])
            for run in runs
        ]

    def box(self, starts, row, octave, near, shift):
        lag = 2**octave
        boxes, shifted = [], []
        for run, z in near:
            pair = []
            for k in range(self.width + 2):
                total = z[k] + self.column(starts, run, k, row, shift)
                pair.append(total * (1.0 / lag) if octave else total)
            ahead = [pltpu.roll(v, LANES - lag, 1) for v in pair]
            if 2 * lag == LANES:
                plus = [
                    jnp.where(self.lane < lag, ahead[k], ahead[k + 1])
                    for k in range(self.width + 1)
                ]
                boxes += [pair[k + 1] + plus[k + 1] for k in range(self.width)]
                shifted += [pair[k + 1] + plus[k] for k in range(self.width)]
            else:
                behind = [pltpu.roll(v, lag, 1) for v in pair]
                for k in range(1, self.width + 1):
                    plus = jnp.where(self.lane < LANES - lag, ahead[k], ahead[k + 1])
                    minus = jnp.where(self.lane >= lag, behind[k], behind[k - 1])
                    boxes.append(pair[k] + plus)
                    shifted.append(pair[k] + minus)
        return boxes, shifted

    def add(self, lags, starts, row, run):
        near = self.near(starts, row, [run])
        count = self.width
        low = run * self.width
        first = second = None
        for octave in range(SCALES):
            shift = self.shift(octave)
            boxes, shifted = self.box(starts, row, octave, near, shift)
            here = row_pad(octave) + row
            for k in range(count):
                lags[octave][0, low + k, pl.ds(pl.multiple_of(here, SUB), SUB), :] = boxes[k]
                lags[octave][1, low + k, pl.ds(pl.multiple_of(here, SUB), SUB), :] = shifted[k]
            past = pl.ds(here - shift, SUB)
            u = [boxes[k] - lags[octave][1, low + k, past, :] for k in range(count)]
            v = [lags[octave][0, low + k, past, :] - shifted[k] for k in range(count)]
            first = u if first is None else [a + b for a, b in zip(first, u)]
            second = v if second is None else [a + b for a, b in zip(second, v)]
        return first, second

    def finish(self, starts, row, first, second, runs=(0, 1)):
        rows = pl.ds(pl.multiple_of(row, SUB), SUB)
        coef = self.coef[rows, :]
        turn = jnp.where(self.top, 1.0, -1.0) * (1.0 / (8.0 * SCALES))
        for k in range(len(runs) * self.width):
            run, within = runs[k // self.width], k % self.width
            column = pl.ds(pl.multiple_of((starts[run] + within) * LANES, LANES), LANES)
            grad_east = (first[k] + second[k]) * coef
            grad_north = (second[k] - first[k]) * turn
            squared = grad_east * grad_east + grad_north * grad_north
            inverse = lax.rsqrt(1.0 + squared)
            sine = squared * lax.rsqrt(jnp.maximum(squared, 1e-37)) * inverse
            ratio = jnp.full_like(inverse, ANGLE[-1])
            for term in ANGLE[-2::-1]:
                ratio = ratio * inverse + term
            self.slope[rows, column] = sine * ratio
            turned = -inverse
            self.facing[0, rows, column] = grad_east * turned
            self.facing[1, rows, column] = grad_north * turned
            tilt = 0.5 * (grad_east - grad_north) + LIGHT_UP
            self.shade[rows, column] = jnp.maximum(tilt * inverse, 0.0)


def run_starts(half, strips):
    quarter = strips // 4
    return (
        jnp.where(half == 0, quarter, 0),
        jnp.where(half == 0, 2 * quarter, 3 * quarter),
    )


def gather(rows, cols, z_ref, strips_ref, part, slope, facing, shade, *scratch):
    lags, (
        rim,
        coef,
        greeted,
        load_sem,
        lat_send,
        lat_recv,
        send_sem,
        recv_sem,
        rim_send,
        rim_recv,
    ) = (
        scratch[:SCALES],
        scratch[SCALES:],
    )
    lat, lon = lax.axis_index("lat"), lax.axis_index("lon")
    n_lat, n_lon = lax.axis_size("lat"), lax.axis_size("lon")
    strips = cols // LANES
    hops = rim_hops(strips)
    width = strips // 4
    count = RUNS * width
    near = near_side(lat)
    far = 1 - near
    exists = (lat > 0, lat < n_lat - 1)
    far_exists = jnp.where(far == 0, exists[0], exists[1])
    far_lat = jnp.where(far == 0, lat - 1, lat + 1)
    near_lat = jnp.where(near == 0, lat - 1, lat + 1)

    def edge(side):
        return pl.multiple_of(jnp.where(side == 0, 0, rows - HALO), SUB)

    def halo(side):
        return pl.multiple_of(jnp.where(side == 0, 0, HALO + rows), SUB)

    def loads_of(number):
        start, size = ((edge(far), HALO), (edge(near), HALO), (HALO, rows - 2 * HALO))[number]
        return [
            pltpu.make_async_copy(
                z_ref.at[pl.ds(start, size), pl.ds(strip * LANES, LANES)],
                strips_ref.at[1 + strip, pl.ds(HALO + start, size), :],
                load_sem.at[number, strip],
            )
            for strip in range(strips)
        ]

    barrier = pltpu.get_barrier_semaphore()

    @pl.when(far_exists)
    def _():
        pl.semaphore_signal(barrier, inc=1, device_id=(far_lat, lon), device_id_type=MESH)

    pl.semaphore_signal(barrier, inc=1, device_id=(near_lat, lon), device_id_type=MESH)

    for number in range(3):
        for load in loads_of(number):
            load.start()

    main = rows - HALO
    base = pl.multiple_of(jnp.where(far == 0, HALO, 0), SUB)
    fill_coef(coef, main, lat * rows + base, rows * n_lat, cols * n_lon)
    for load in loads_of(0):
        load.wait()
    odd = lax.rem(lon, 2)
    leads = odd == 0
    follows = odd == 1
    pl.semaphore_wait(barrier, 1 + far_exists.astype(jnp.int32) + len(hops) * odd)

    @pl.when(leads)
    def _():
        for hop, _ in hops:
            pl.semaphore_signal(barrier, inc=1, device_id=(lat, hop), device_id_type=MESH)

    @pl.when(follows)
    def _():
        for hop, _ in hops:
            pl.semaphore_signal(greeted, inc=1, device_id=(lat, hop), device_id_type=MESH)


    quarter = strips // 4
    pieces = ((1, quarter), (1 + quarter, strips - quarter))

    def lat_copy(distant, piece):
        side, other = (far, far_lat) if distant else (near, near_lat)
        part_ = pl.ds(*piece)
        index = pieces.index(piece)
        return pltpu.make_async_remote_copy(
            src_ref=strips_ref.at[part_, pl.ds(HALO + edge(side), HALO), :],
            dst_ref=strips_ref.at[part_, pl.ds(halo(1 - side), HALO), :],
            send_sem=lat_send.at[distant, index],
            recv_sem=lat_recv.at[distant, index],
            device_id=(other, lon),
            device_id_type=MESH,
        )

    def corner_copy(distant, index):
        side, other = (far, far_lat) if distant else (near, near_lat)
        hop, target = hops[index]
        return pltpu.make_async_remote_copy(
            src_ref=rim.at[pl.ds(edge(side), HALO), :],
            dst_ref=strips_ref.at[target, pl.ds(halo(1 - side), HALO), :],
            send_sem=send_sem.at[distant, index],
            recv_sem=recv_sem.at[distant, index],
            device_id=(other, hop),
            device_id_type=MESH,
        )

    def rim_copy(index):
        hop, target = hops[index]
        return pltpu.make_async_remote_copy(
            src_ref=rim,
            dst_ref=strips_ref.at[target, pl.ds(HALO, rows), :],
            send_sem=rim_send.at[index],
            recv_sem=rim_recv.at[index],
            device_id=(lat, hop),
            device_id_type=MESH,
        )

    def arrived(distant, piece=None, index=0):
        here = pl.ds(halo(far if distant else near), HALO)
        if piece is None:
            place = strips_ref.at[hops[index][1], here, :]
            sends, receives = send_sem, recv_sem
        else:
            place = strips_ref.at[pl.ds(*piece), here, :]
            sends, receives, index = lat_send, lat_recv, pieces.index(piece)
        pltpu.make_async_remote_copy(
            src_ref=place,
            dst_ref=place,
            send_sem=sends.at[distant, index],
            recv_sem=receives.at[distant, index],
            device_id=(lat, hops[0][0]),
            device_id_type=MESH,
        ).wait_recv()

    @pl.when(far_exists)
    def _():
        lat_copy(1, pieces[0]).start()

    for load in loads_of(1):
        load.wait()
    for piece in pieces:
        lat_copy(0, piece).start()
    for load in loads_of(2):
        load.wait()
    lane = lax.broadcasted_iota(jnp.int32, (SUB, LANES), 1)
    for start in range(0, rows, SUB):
        here = pl.ds(HALO + start, SUB)
        rim[pl.ds(start, SUB), :] = jnp.where(
            lane < HALO, strips_ref[1, here, :], strips_ref[strips, here, :]
        )

    for octave in range(SCALES):
        pad = row_pad(octave)
        first = pl.multiple_of(jnp.where(far == 0, 0, pad + rows), SUB)
        for k in range(count):
            for start in range(0, pad, SUB):
                for which in range(2):
                    lags[octave][which, k, pl.ds(first + start, SUB), :] = jnp.zeros(
                        (SUB, LANES), jnp.float32
                    )

    def send_rims():
        for index in range(len(hops)):
            rim_copy(index).start()
            corner_copy(0, index).start()

        @pl.when(far_exists)
        def _():
            for index in range(len(hops)):
                corner_copy(1, index).start()

    pl.when(follows)(send_rims)

    @pl.when(far_exists)
    def _():
        lat_copy(1, pieces[1]).start()

    window = Window(strips_ref, rows, strips, far, coef, slope, facing, shade)
    far_base = pl.multiple_of(jnp.where(far == 0, 0, main), SUB)

    def half(number, carry):
        @pl.when(number == 1)
        def _():
            for index in range(len(hops)):
                rim_copy(index).wait_recv()
                arrived(0, index=index)

        starts = run_starts(number, strips)

        def partly(block, carry):
            for inner in range(UNROLL):
                row = window.row(block * UNROLL + inner)
                rows_here = pl.ds(pl.multiple_of(row - far_base, SUB), SUB)
                for run in range(RUNS):
                    found = window.add(lags, starts, row, run)
                    for which in range(2):
                        for k in range(width):
                            part[which, starts[run] + k, rows_here, :] = found[which][k]
            return carry

        def fully(block, carry):
            for inner in range(UNROLL):
                row = window.row(block * UNROLL + inner)
                for run in range(RUNS):
                    window.finish(
                        starts, row - base, *window.add(lags, starts, row, run), runs=(run,)
                    )
            return carry

        size = UNROLL * SUB
        lax.fori_loop(0, HALO // size, partly, 0)

        @pl.when(jnp.logical_and(number == 0, leads))
        def _():
            pl.semaphore_wait(greeted, len(hops))
            send_rims()

        @pl.when(number == 0)
        def _():
            for piece in pieces:
                arrived(0, piece)

        lax.fori_loop(HALO // size, rows // size, fully, 0)
        return carry

    lax.fori_loop(0, 2, half, 0)

    for pole in range(2):

        @pl.when(jnp.logical_and(jnp.logical_not(far_exists), far == pole))
        def _():
            first = HALO if pole == 0 else HALO + rows - SUB
            pick = 0 if pole == 0 else SUB - 1
            fill = 0 if pole == 0 else HALO + rows

            def repeat(strip, carry):
                row = strips_ref[strip, pl.ds(first, SUB), :][pick : pick + 1]
                block = jnp.broadcast_to(row, (SUB, LANES))
                for k in range(HALO // SUB):
                    strips_ref[strip, pl.ds(fill + k * SUB, SUB), :] = block
                return carry

            lax.fori_loop(0, strips_ref.shape[0], repeat, 0)

    for piece in pieces:
        lat_copy(0, piece).wait_send()
    for index in range(len(hops)):
        rim_copy(index).wait_send()
        corner_copy(0, index).wait_send()

    @pl.when(far_exists)
    def _():
        for piece in pieces:
            lat_copy(1, piece).wait_send()
            arrived(1, piece)
        for index in range(len(hops)):
            corner_copy(1, index).wait_send()
            arrived(1, index=index)


def shade_far(rows, cols, *refs):
    strips_ref, part, slope, facing, shade, slope_out, facing_out, shade_out = refs[:8]
    coef, slope_far, facing_far, shade_far_, near_sem, far_sem = refs[8:]
    lat = lax.axis_index("lat")
    n_lat, n_lon = lax.axis_size("lat"), lax.axis_size("lon")
    far = 1 - near_side(lat)
    strips = cols // LANES
    width = strips // 4
    count = RUNS * width
    main = rows - HALO
    base = pl.multiple_of(jnp.where(far == 0, HALO, 0), SUB)
    far_base = pl.multiple_of(jnp.where(far == 0, 0, main), SUB)
    done = [
        pltpu.make_async_copy(source, target, near_sem.at[index])
        for index, (source, target) in enumerate(
            (
                (slope, slope_out.at[pl.ds(base, main), :]),
                (shade, shade_out.at[pl.ds(base, main), :]),
                (facing.at[0], facing_out.at[0, pl.ds(base, main), :]),
                (facing.at[1], facing_out.at[1, pl.ds(base, main), :]),
            )
        )
    ]
    for copy in done:
        copy.start()
    fill_coef(coef, HALO, lat * rows + far_base, rows * n_lat, cols * n_lon)
    window = Window(strips_ref, rows, strips, far, coef, slope_far, facing_far, shade_far_)
    sublane = lax.broadcasted_iota(jnp.int32, (SUB, LANES), 0)

    def copies(number):
        found = []
        for run, start in enumerate(run_starts(number, strips)):
            column = pl.ds(pl.multiple_of(start * LANES, LANES), width * LANES)
            here = pl.ds(far_base, HALO)
            for index, (source, target) in enumerate(
                (
                    (slope_far.at[:, column], slope_out.at[here, column]),
                    (shade_far_.at[:, column], shade_out.at[here, column]),
                    (facing_far.at[0, :, column], facing_out.at[0, here, column]),
                    (facing_far.at[1, :, column], facing_out.at[1, here, column]),
                )
            ):
                found.append(
                    pltpu.make_async_copy(source, target, far_sem.at[number, run, index])
                )
        return found

    def half(number, carry):
        starts = run_starts(number, strips)
        for step in range(HALO // SUB):
            row = window.row(step)
            local_row = pl.multiple_of(row - far_base, SUB)
            first, second = [
                [
                    part[which, starts[k // width] + k % width, pl.ds(local_row, SUB), :]
                    for k in range(count)
                ]
                for which in range(2)
            ]
            near = window.near(starts, row, range(RUNS))
            for octave in range(SCALES):
                lag = 2**octave
                if row_pad(octave) <= step * SUB:
                    continue
                boxes, shifted = window.box(starts, row, octave, near, -window.shift(octave))
                if lag < SUB:
                    beyond = jnp.logical_or(
                        jnp.logical_and(far == 0, sublane < lag),
                        jnp.logical_and(far == 1, sublane >= SUB - lag),
                    )
                    boxes = [jnp.where(beyond, v, 0.0) for v in boxes]
                    shifted = [jnp.where(beyond, v, 0.0) for v in shifted]
                first = [a - b for a, b in zip(first, shifted)]
                second = [a + b for a, b in zip(second, boxes)]
            window.finish(starts, local_row, first, second)
        for copy in copies(number):
            copy.start()
        return carry

    lax.fori_loop(0, 2, half, 0)
    for copy in done:
        copy.wait()
    for number in range(2):
        for copy in copies(number):
            copy.wait()


def local(elevation):
    rows, cols = elevation.shape
    strips = cols // LANES
    count = RUNS * (strips // 4)
    hops = 1 if lax.axis_size("lon") == 2 else 2
    main = rows - HALO
    vmem = pl.BlockSpec(memory_space=pltpu.VMEM)
    anywhere = pl.BlockSpec(memory_space=pl.ANY)
    staged = pl.pallas_call(
        functools.partial(gather, rows, cols),
        out_shape=(
            pltpu.VMEM((strips + hops, spread(rows + 2 * HALO), LANES), jnp.float32),
            pltpu.VMEM((2, strips, HALO, LANES), jnp.float32),
            pltpu.VMEM((main, cols), jnp.float32),
            pltpu.VMEM((2, main, cols), jnp.float32),
            pltpu.VMEM((main, cols), jnp.float32),
        ),
        in_specs=[anywhere],
        out_specs=(vmem,) * 5,
        scratch_shapes=[
            pltpu.VMEM((2, count, spread(rows + 2 * row_pad(k)), LANES), jnp.float32)
            for k in range(SCALES)
        ]
        + [
            pltpu.VMEM((rows, LANES), jnp.float32),
            pltpu.VMEM((main, LANES), jnp.float32),
            pltpu.SemaphoreType.REGULAR,
            pltpu.SemaphoreType.DMA((3, strips)),
            pltpu.SemaphoreType.DMA((2, 2)),
            pltpu.SemaphoreType.DMA((2, 2)),
            pltpu.SemaphoreType.DMA((2, hops)),
            pltpu.SemaphoreType.DMA((2, hops)),
            pltpu.SemaphoreType.DMA((hops,)),
            pltpu.SemaphoreType.DMA((hops,)),
        ],
        compiler_params=pltpu.CompilerParams(
            collective_id=0, has_side_effects=True, vmem_limit_bytes=52 * 2**20
        ),
    )(elevation)
    return tuple(
        pl.pallas_call(
            functools.partial(shade_far, rows, cols),
            out_shape=(
                jax.ShapeDtypeStruct((rows, cols), jnp.float32),
                jax.ShapeDtypeStruct((2, rows, cols), jnp.float32),
                jax.ShapeDtypeStruct((rows, cols), jnp.float32),
            ),
            in_specs=[vmem] * 5,
            out_specs=(anywhere,) * 3,
            scratch_shapes=[
                pltpu.VMEM((HALO, LANES), jnp.float32),
                pltpu.VMEM((HALO, cols), jnp.float32),
                pltpu.VMEM((2, HALO, cols), jnp.float32),
                pltpu.VMEM((HALO, cols), jnp.float32),
                pltpu.SemaphoreType.DMA((4,)),
                pltpu.SemaphoreType.DMA((2, RUNS, 4)),
            ],
            compiler_params=pltpu.CompilerParams(vmem_limit_bytes=16 * 2**20),
        )(*staged)
    )


def solution(mesh):
    in_specs = (P("lat", "lon"),)
    out_specs = (P("lat", "lon"), P(None, "lat", "lon"), P("lat", "lon"))
    return jax.shard_map(local, mesh=mesh, in_specs=in_specs, out_specs=out_specs, check_vma=False)
```

```python
import functools
import math

import jax
import jax.numpy as jnp
from jax import lax
from jax.experimental import pallas as pl
from jax.experimental.pallas import tpu as pltpu
from jax.sharding import PartitionSpec as P

SCALES = 7
HALO = 64
LANES = 128
SUB = 8
RUNS = 2
UNROLL = 4

LIGHT_UP = math.sqrt(0.5)
MESH = pl.DeviceIdType.MESH

ANGLE = (
    1.5707962050889646,
    -0.9999801696091738,
    0.7848538132927688,
    -0.6607586188432167,
    0.5557489578459907,
    -0.42189571811945836,
    0.2501265286961767,
    -0.09607630454800326,
    0.01718536914918157,
)


def spread(rows):
    return rows + (-rows // SUB + 1) % 4 * SUB


def row_pad(octave):
    return max(2**octave, SUB)


def rim_hops(strips):
    lon, n_lon = lax.axis_index("lon"), lax.axis_size("lon")
    hops = [(lax.rem(lon + 1, n_lon), 0)]
    if n_lon > 2:
        hops.append((lax.rem(lon + n_lon - 1, n_lon), strips + 1))
    return hops


def east_halo(strips):
    return strips + 1 if lax.axis_size("lon") > 2 else 0


def near_side(lat):
    return 1 - lax.rem(lat, 2)


def fill_coef(coef_ref, count, first_row, total_rows, total_cols):
    for start in range(0, count, SUB):
        position = first_row + start + lax.broadcasted_iota(jnp.int32, (SUB, LANES), 0)
        spacing = jnp.sin((position.astype(jnp.float32) + 0.5) * (math.pi / total_rows)) * (
            2.0 * total_rows / total_cols
        )
        coef_ref[pl.ds(start, SUB), :] = 1.0 / (8.0 * SCALES * spacing)


class Window:
    def __init__(self, strips, rows, columns, far, coef, slope, facing, shade):
        self.strips, self.rows, self.columns = strips, rows, columns
        self.width = columns // 4
        self.coef, self.slope, self.facing, self.shade = coef, slope, facing, shade
        self.top = far == 0
        self.sign = jnp.where(self.top, 1, -1)
        self.lane = lax.broadcasted_iota(jnp.int32, (SUB, LANES), 1)

    def row(self, number):
        return pl.multiple_of(
            jnp.where(self.top, number * SUB, self.rows - SUB - number * SUB), SUB
        )

    def shift(self, octave):
        lag = 2**octave
        moved = self.sign * lag
        return pl.multiple_of(moved, SUB) if lag >= SUB else moved

    def column(self, starts, run, offset, row, shift=0):
        place = pl.ds(HALO + row + shift, SUB)
        strip = starts[run] + offset
        if offset == self.width + 1:
            strip = jnp.where(strip > self.columns, east_halo(self.columns), strip)
        return self.strips[strip, place, :]

    def near(self, starts, row, runs):
        return [
            (run, [self.column(starts, run, k, row) for k in range(self.width + 2)])
            for run in runs
        ]

    def box(self, starts, row, octave, near, shift):
        lag = 2**octave
        boxes, shifted = [], []
        for run, z in near:
            pair = []
            for k in range(self.width + 2):
                total = z[k] + self.column(starts, run, k, row, shift)
                pair.append(total * (1.0 / lag) if octave else total)
            ahead = [pltpu.roll(v, LANES - lag, 1) for v in pair]
            if 2 * lag == LANES:
                plus = [
                    jnp.where(self.lane < lag, ahead[k], ahead[k + 1])
                    for k in range(self.width + 1)
                ]
                boxes += [pair[k + 1] + plus[k + 1] for k in range(self.width)]
                shifted += [pair[k + 1] + plus[k] for k in range(self.width)]
            else:
                behind = [pltpu.roll(v, lag, 1) for v in pair]
                for k in range(1, self.width + 1):
                    plus = jnp.where(self.lane < LANES - lag, ahead[k], ahead[k + 1])
                    minus = jnp.where(self.lane >= lag, behind[k], behind[k - 1])
                    boxes.append(pair[k] + plus)
                    shifted.append(pair[k] + minus)
        return boxes, shifted

    def add(self, lags, starts, row, run):
        near = self.near(starts, row, [run])
        count = self.width
        low = run * self.width
        first = second = None
        for octave in range(SCALES):
            shift = self.shift(octave)
            boxes, shifted = self.box(starts, row, octave, near, shift)
            here = row_pad(octave) + row
            for k in range(count):
                lags[octave][0, low + k, pl.ds(pl.multiple_of(here, SUB), SUB), :] = boxes[k]
                lags[octave][1, low + k, pl.ds(pl.multiple_of(here, SUB), SUB), :] = shifted[k]
            past = pl.ds(here - shift, SUB)
            u = [boxes[k] - lags[octave][1, low + k, past, :] for k in range(count)]
            v = [lags[octave][0, low + k, past, :] - shifted[k] for k in range(count)]
            first = u if first is None else [a + b for a, b in zip(first, u)]
            second = v if second is None else [a + b for a, b in zip(second, v)]
        return first, second

    def finish(self, starts, row, first, second, runs=(0, 1)):
        rows = pl.ds(pl.multiple_of(row, SUB), SUB)
        coef = self.coef[rows, :]
        turn = jnp.where(self.top, 1.0, -1.0) * (1.0 / (8.0 * SCALES))
        for k in range(len(runs) * self.width):
            run, within = runs[k // self.width], k % self.width
            column = pl.ds(pl.multiple_of((starts[run] + within) * LANES, LANES), LANES)
            grad_east = (first[k] + second[k]) * coef
            grad_north = (second[k] - first[k]) * turn
            squared = grad_east * grad_east + grad_north * grad_north
            inverse = lax.rsqrt(1.0 + squared)
            sine = squared * lax.rsqrt(jnp.maximum(squared, 1e-37)) * inverse
            ratio = jnp.full_like(inverse, ANGLE[-1])
            for term in ANGLE[-2::-1]:
                ratio = ratio * inverse + term
            self.slope[rows, column] = sine * ratio
            turned = -inverse
            self.facing[0, rows, column] = grad_east * turned
            self.facing[1, rows, column] = grad_north * turned
            tilt = 0.5 * (grad_east - grad_north) + LIGHT_UP
            self.shade[rows, column] = jnp.maximum(tilt * inverse, 0.0)


def run_starts(half, strips):
    quarter = strips // 4
    return (
        jnp.where(half == 0, quarter, 0),
        jnp.where(half == 0, 2 * quarter, 3 * quarter),
    )


def gather(rows, cols, z_ref, strips_ref, part, slope, facing, shade, *scratch):
    lags, (
        rim,
        far_rim,
        coef,
        greeted,
        load_sem,
        lat_send,
        lat_recv,
        send_sem,
        recv_sem,
        rim_send,
        rim_recv,
    ) = (
        scratch[:SCALES],
        scratch[SCALES:],
    )
    lat, lon = lax.axis_index("lat"), lax.axis_index("lon")
    n_lat, n_lon = lax.axis_size("lat"), lax.axis_size("lon")
    strips = cols // LANES
    hops = rim_hops(strips)
    width = strips // 4
    count = RUNS * width
    near = near_side(lat)
    far = 1 - near
    exists = (lat > 0, lat < n_lat - 1)
    far_exists = jnp.where(far == 0, exists[0], exists[1])
    far_lat = jnp.where(far == 0, lat - 1, lat + 1)
    near_lat = jnp.where(near == 0, lat - 1, lat + 1)

    def edge(side):
        return pl.multiple_of(jnp.where(side == 0, 0, rows - HALO), SUB)

    def halo(side):
        return pl.multiple_of(jnp.where(side == 0, 0, HALO + rows), SUB)

    def loads_of(number):
        start, size = ((edge(far), HALO), (edge(near), HALO), (HALO, rows - 2 * HALO))[number]
        return [
            pltpu.make_async_copy(
                z_ref.at[pl.ds(start, size), pl.ds(strip * LANES, LANES)],
                strips_ref.at[1 + strip, pl.ds(HALO + start, size), :],
                load_sem.at[number, strip],
            )
            for strip in range(strips)
        ]

    barrier = pltpu.get_barrier_semaphore()

    @pl.when(far_exists)
    def _():
        pl.semaphore_signal(barrier, inc=1, device_id=(far_lat, lon), device_id_type=MESH)

    pl.semaphore_signal(barrier, inc=1, device_id=(near_lat, lon), device_id_type=MESH)

    for number in range(3):
        for load in loads_of(number):
            load.start()

    main = rows - HALO
    base = pl.multiple_of(jnp.where(far == 0, HALO, 0), SUB)
    fill_coef(coef, main, lat * rows + base, rows * n_lat, cols * n_lon)
    for load in loads_of(0):
        load.wait()
    odd = lax.rem(lon, 2)
    leads = odd == 0
    follows = odd == 1
    pl.semaphore_wait(barrier, 1 + far_exists.astype(jnp.int32) + len(hops) * odd)

    @pl.when(leads)
    def _():
        for hop, _ in hops:
            pl.semaphore_signal(barrier, inc=1, device_id=(lat, hop), device_id_type=MESH)

    @pl.when(follows)
    def _():
        for hop, _ in hops:
            pl.semaphore_signal(greeted, inc=1, device_id=(lat, hop), device_id_type=MESH)


    pieces = ((1, 1), (strips, 1), (2, strips - 2))

    def lat_copy(distant, piece):
        side, other = (far, far_lat) if distant else (near, near_lat)
        part_ = pl.ds(*piece)
        index = pieces.index(piece)
        return pltpu.make_async_remote_copy(
            src_ref=strips_ref.at[part_, pl.ds(HALO + edge(side), HALO), :],
            dst_ref=strips_ref.at[part_, pl.ds(halo(1 - side), HALO), :],
            send_sem=lat_send.at[distant, index],
            recv_sem=lat_recv.at[distant, index],
            device_id=(other, lon),
            device_id_type=MESH,
        )

    def corner_copy(distant, index):
        hop, target = hops[index]
        source, row, other = (
            (far_rim, halo(far), lat) if distant else (rim, halo(far), near_lat)
        )
        source = source if distant else source.at[pl.ds(edge(near), HALO), :]
        return pltpu.make_async_remote_copy(
            src_ref=source,
            dst_ref=strips_ref.at[target, pl.ds(row, HALO), :],
            send_sem=send_sem.at[distant, index],
            recv_sem=recv_sem.at[distant, index],
            device_id=(other, hop),
            device_id_type=MESH,
        )

    def rim_copy(index):
        hop, target = hops[index]
        return pltpu.make_async_remote_copy(
            src_ref=rim,
            dst_ref=strips_ref.at[target, pl.ds(HALO, rows), :],
            send_sem=rim_send.at[index],
            recv_sem=rim_recv.at[index],
            device_id=(lat, hop),
            device_id_type=MESH,
        )

    def arrived(distant, piece=None, index=0):
        here = pl.ds(halo(far if distant else near), HALO)
        if piece is None:
            place = strips_ref.at[hops[index][1], here, :]
            sends, receives = send_sem, recv_sem
        else:
            place = strips_ref.at[pl.ds(*piece), here, :]
            sends, receives, index = lat_send, lat_recv, pieces.index(piece)
        pltpu.make_async_remote_copy(
            src_ref=place,
            dst_ref=place,
            send_sem=sends.at[distant, index],
            recv_sem=receives.at[distant, index],
            device_id=(lat, hops[0][0]),
            device_id_type=MESH,
        ).wait_recv()

    @pl.when(far_exists)
    def _():
        for piece in pieces:
            lat_copy(1, piece).start()

    for load in loads_of(1):
        load.wait()
    for piece in pieces:
        lat_copy(0, piece).start()
    for load in loads_of(2):
        load.wait()
    lane = lax.broadcasted_iota(jnp.int32, (SUB, LANES), 1)
    for start in range(0, rows, SUB):
        here = pl.ds(HALO + start, SUB)
        rim[pl.ds(start, SUB), :] = jnp.where(
            lane < HALO, strips_ref[1, here, :], strips_ref[strips, here, :]
        )

    for octave in range(SCALES):
        pad = row_pad(octave)
        first = pl.multiple_of(jnp.where(far == 0, 0, pad + rows), SUB)
        for k in range(count):
            for start in range(0, pad, SUB):
                for which in range(2):
                    lags[octave][which, k, pl.ds(first + start, SUB), :] = jnp.zeros(
                        (SUB, LANES), jnp.float32
                    )

    def send_rims():
        for index in range(len(hops)):
            rim_copy(index).start()
            corner_copy(0, index).start()

    pl.when(follows)(send_rims)


    window = Window(strips_ref, rows, strips, far, coef, slope, facing, shade)
    far_base = pl.multiple_of(jnp.where(far == 0, 0, main), SUB)

    def half(number, carry):
        @pl.when(number == 1)
        def _():
            for index in range(len(hops)):
                rim_copy(index).wait_recv()
                arrived(0, index=index)

        starts = run_starts(number, strips)

        def partly(block, carry):
            for inner in range(UNROLL):
                row = window.row(block * UNROLL + inner)
                rows_here = pl.ds(pl.multiple_of(row - far_base, SUB), SUB)
                for run in range(RUNS):
                    found = window.add(lags, starts, row, run)
                    for which in range(2):
                        for k in range(width):
                            part[which, starts[run] + k, rows_here, :] = found[which][k]
            return carry

        def fully(block, carry):
            for inner in range(UNROLL):
                row = window.row(block * UNROLL + inner)
                for run in range(RUNS):
                    window.finish(
                        starts, row - base, *window.add(lags, starts, row, run), runs=(run,)
                    )
            return carry

        size = UNROLL * SUB
        lax.fori_loop(0, HALO // size, partly, 0)

        @pl.when(jnp.logical_and(number == 0, leads))
        def _():
            pl.semaphore_wait(greeted, len(hops))
            send_rims()

        @pl.when(number == 0)
        def _():
            for piece in pieces:
                arrived(0, piece)

        def segment(index, carry):
            outer = jnp.logical_and(number == 1, far_exists)

            @pl.when(jnp.logical_and(outer, index == 0))
            def _():
                for piece in pieces[:2]:
                    arrived(1, piece)
                for start in range(0, HALO, SUB):
                    here = pl.ds(pl.multiple_of(halo(far) + start, SUB), SUB)
                    far_rim[pl.ds(start, SUB), :] = jnp.where(
                        lane < HALO, strips_ref[1, here, :], strips_ref[strips, here, :]
                    )

            @pl.when(jnp.logical_and(outer, index == 1))
            def _():
                for hop in range(len(hops)):
                    corner_copy(1, hop).start()

            first = HALO // size
            low = jnp.where(index == 0, first, first + 1)
            high = jnp.where(index == 0, first + 1, rows // size)
            lax.fori_loop(low, high, fully, 0)
            return carry

        lax.fori_loop(0, 2, segment, 0)
        return carry

    lax.fori_loop(0, 2, half, 0)

    for pole in range(2):

        @pl.when(jnp.logical_and(jnp.logical_not(far_exists), far == pole))
        def _():
            first = HALO if pole == 0 else HALO + rows - SUB
            pick = 0 if pole == 0 else SUB - 1
            fill = 0 if pole == 0 else HALO + rows

            def repeat(strip, carry):
                row = strips_ref[strip, pl.ds(first, SUB), :][pick : pick + 1]
                block = jnp.broadcast_to(row, (SUB, LANES))
                for k in range(HALO // SUB):
                    strips_ref[strip, pl.ds(fill + k * SUB, SUB), :] = block
                return carry

            lax.fori_loop(0, strips_ref.shape[0], repeat, 0)

    for piece in pieces:
        lat_copy(0, piece).wait_send()
    for index in range(len(hops)):
        rim_copy(index).wait_send()
        corner_copy(0, index).wait_send()

    @pl.when(far_exists)
    def _():
        for piece in pieces:
            lat_copy(1, piece).wait_send()
        arrived(1, pieces[2])
        for index in range(len(hops)):
            corner_copy(1, index).wait_send()
            arrived(1, index=index)


def shade_far(rows, cols, *refs):
    strips_ref, part, slope, facing, shade, slope_out, facing_out, shade_out = refs[:8]
    coef, slope_far, facing_far, shade_far_, near_sem, far_sem = refs[8:]
    lat = lax.axis_index("lat")
    n_lat, n_lon = lax.axis_size("lat"), lax.axis_size("lon")
    far = 1 - near_side(lat)
    strips = cols // LANES
    width = strips // 4
    count = RUNS * width
    main = rows - HALO
    base = pl.multiple_of(jnp.where(far == 0, HALO, 0), SUB)
    far_base = pl.multiple_of(jnp.where(far == 0, 0, main), SUB)
    done = [
        pltpu.make_async_copy(source, target, near_sem.at[index])
        for index, (source, target) in enumerate(
            (
                (slope, slope_out.at[pl.ds(base, main), :]),
                (shade, shade_out.at[pl.ds(base, main), :]),
                (facing.at[0], facing_out.at[0, pl.ds(base, main), :]),
                (facing.at[1], facing_out.at[1, pl.ds(base, main), :]),
            )
        )
    ]
    for copy in done:
        copy.start()
    fill_coef(coef, HALO, lat * rows + far_base, rows * n_lat, cols * n_lon)
    window = Window(strips_ref, rows, strips, far, coef, slope_far, facing_far, shade_far_)
    sublane = lax.broadcasted_iota(jnp.int32, (SUB, LANES), 0)

    def copies(number):
        found = []
        for run, start in enumerate(run_starts(number, strips)):
            column = pl.ds(pl.multiple_of(start * LANES, LANES), width * LANES)
            here = pl.ds(far_base, HALO)
            for index, (source, target) in enumerate(
                (
                    (slope_far.at[:, column], slope_out.at[here, column]),
                    (shade_far_.at[:, column], shade_out.at[here, column]),
                    (facing_far.at[0, :, column], facing_out.at[0, here, column]),
                    (facing_far.at[1, :, column], facing_out.at[1, here, column]),
                )
            ):
                found.append(
                    pltpu.make_async_copy(source, target, far_sem.at[number, run, index])
                )
        return found

    def half(number, carry):
        starts = run_starts(number, strips)
        for step in range(HALO // SUB):
            row = window.row(step)
            local_row = pl.multiple_of(row - far_base, SUB)
            first, second = [
                [
                    part[which, starts[k // width] + k % width, pl.ds(local_row, SUB), :]
                    for k in range(count)
                ]
                for which in range(2)
            ]
            near = window.near(starts, row, range(RUNS))
            for octave in range(SCALES):
                lag = 2**octave
                if row_pad(octave) <= step * SUB:
                    continue
                boxes, shifted = window.box(starts, row, octave, near, -window.shift(octave))
                if lag < SUB:
                    beyond = jnp.logical_or(
                        jnp.logical_and(far == 0, sublane < lag),
                        jnp.logical_and(far == 1, sublane >= SUB - lag),
                    )
                    boxes = [jnp.where(beyond, v, 0.0) for v in boxes]
                    shifted = [jnp.where(beyond, v, 0.0) for v in shifted]
                first = [a - b for a, b in zip(first, shifted)]
                second = [a + b for a, b in zip(second, boxes)]
            window.finish(starts, local_row, first, second)
        for copy in copies(number):
            copy.start()
        return carry

    lax.fori_loop(0, 2, half, 0)
    for copy in done:
        copy.wait()
    for number in range(2):
        for copy in copies(number):
            copy.wait()


def local(elevation):
    rows, cols = elevation.shape
    strips = cols // LANES
    count = RUNS * (strips // 4)
    hops = 1 if lax.axis_size("lon") == 2 else 2
    main = rows - HALO
    vmem = pl.BlockSpec(memory_space=pltpu.VMEM)
    anywhere = pl.BlockSpec(memory_space=pl.ANY)
    staged = pl.pallas_call(
        functools.partial(gather, rows, cols),
        out_shape=(
            pltpu.VMEM((strips + hops, spread(rows + 2 * HALO), LANES), jnp.float32),
            pltpu.VMEM((2, strips, HALO, LANES), jnp.float32),
            pltpu.VMEM((main, cols), jnp.float32),
            pltpu.VMEM((2, main, cols), jnp.float32),
            pltpu.VMEM((main, cols), jnp.float32),
        ),
        in_specs=[anywhere],
        out_specs=(vmem,) * 5,
        scratch_shapes=[
            pltpu.VMEM((2, count, spread(rows + 2 * row_pad(k)), LANES), jnp.float32)
            for k in range(SCALES)
        ]
        + [
            pltpu.VMEM((rows, LANES), jnp.float32),
            pltpu.VMEM((HALO, LANES), jnp.float32),
            pltpu.VMEM((main, LANES), jnp.float32),
            pltpu.SemaphoreType.REGULAR,
            pltpu.SemaphoreType.DMA((3, strips)),
            pltpu.SemaphoreType.DMA((2, 3)),
            pltpu.SemaphoreType.DMA((2, 3)),
            pltpu.SemaphoreType.DMA((2, hops)),
            pltpu.SemaphoreType.DMA((2, hops)),
            pltpu.SemaphoreType.DMA((hops,)),
            pltpu.SemaphoreType.DMA((hops,)),
        ],
        compiler_params=pltpu.CompilerParams(
            collective_id=0, has_side_effects=True, vmem_limit_bytes=52 * 2**20
        ),
    )(elevation)
    return tuple(
        pl.pallas_call(
            functools.partial(shade_far, rows, cols),
            out_shape=(
                jax.ShapeDtypeStruct((rows, cols), jnp.float32),
                jax.ShapeDtypeStruct((2, rows, cols), jnp.float32),
                jax.ShapeDtypeStruct((rows, cols), jnp.float32),
            ),
            in_specs=[vmem] * 5,
            out_specs=(anywhere,) * 3,
            scratch_shapes=[
                pltpu.VMEM((HALO, LANES), jnp.float32),
                pltpu.VMEM((HALO, cols), jnp.float32),
                pltpu.VMEM((2, HALO, cols), jnp.float32),
                pltpu.VMEM((HALO, cols), jnp.float32),
                pltpu.SemaphoreType.DMA((4,)),
                pltpu.SemaphoreType.DMA((2, RUNS, 4)),
            ],
            compiler_params=pltpu.CompilerParams(vmem_limit_bytes=16 * 2**20),
        )(*staged)
    )


def solution(mesh):
    in_specs = (P("lat", "lon"),)
    out_specs = (P("lat", "lon"), P(None, "lat", "lon"), P("lat", "lon"))
    return jax.shard_map(local, mesh=mesh, in_specs=in_specs, out_specs=out_specs, check_vma=False)
```

```python
import functools
import math

import jax
import jax.numpy as jnp
from jax import lax
from jax.experimental import pallas as pl
from jax.experimental.pallas import tpu as pltpu
from jax.sharding import PartitionSpec as P

SCALES = 7
HALO = 64
LANES = 128
SUB = 8
RUNS = 2
UNROLL = 4

LIGHT_UP = math.sqrt(0.5)
MESH = pl.DeviceIdType.MESH

ANGLE = (
    1.5707962050889646,
    -0.9999801696091738,
    0.7848538132927688,
    -0.6607586188432167,
    0.5557489578459907,
    -0.42189571811945836,
    0.2501265286961767,
    -0.09607630454800326,
    0.01718536914918157,
)


def spread(rows):
    return rows + (-rows // SUB + 1) % 4 * SUB


def row_pad(octave):
    return max(2**octave, SUB)


def rim_hops(strips):
    lon, n_lon = lax.axis_index("lon"), lax.axis_size("lon")
    hops = [(lax.rem(lon + 1, n_lon), 0)]
    if n_lon > 2:
        hops.append((lax.rem(lon + n_lon - 1, n_lon), strips + 1))
    return hops


def east_halo(strips):
    return strips + 1 if lax.axis_size("lon") > 2 else 0


def near_side(lat):
    return 1 - lax.rem(lat, 2)


def fill_coef(coef_ref, count, first_row, total_rows, total_cols):
    row = lax.broadcasted_iota(jnp.int32, (SUB, LANES), 0)
    tile = jnp.minimum(lax.broadcasted_iota(jnp.int32, (SUB, LANES), 1), count // SUB - 1)
    position = first_row + row + tile * SUB
    spacing = jnp.sin((position.astype(jnp.float32) + 0.5) * (math.pi / total_rows)) * (
        2.0 * total_rows / total_cols
    )
    coef = 1.0 / (8.0 * SCALES * spacing)
    for number in range(count // SUB):
        coef_ref[pl.ds(number * SUB, SUB), :] = jnp.broadcast_to(
            coef[:, number : number + 1], (SUB, LANES)
        )


class Window:
    def __init__(self, strips, rows, columns, far, coef, slope, facing, shade):
        self.strips, self.rows, self.columns = strips, rows, columns
        self.width = columns // 4
        self.coef, self.slope, self.facing, self.shade = coef, slope, facing, shade
        self.top = far == 0
        self.sign = jnp.where(self.top, 1, -1)
        self.lane = lax.broadcasted_iota(jnp.int32, (SUB, LANES), 1)

    def row(self, number):
        return pl.multiple_of(
            jnp.where(self.top, number * SUB, self.rows - SUB - number * SUB), SUB
        )

    def shift(self, octave):
        lag = 2**octave
        moved = self.sign * lag
        return pl.multiple_of(moved, SUB) if lag >= SUB else moved

    def column(self, starts, run, offset, row, shift=0):
        place = pl.ds(HALO + row + shift, SUB)
        strip = starts[run] + offset
        if offset == self.width + 1:
            strip = jnp.where(strip > self.columns, east_halo(self.columns), strip)
        return self.strips[strip, place, :]

    def near(self, starts, row, runs):
        return [
            (run, [self.column(starts, run, k, row) for k in range(self.width + 2)])
            for run in runs
        ]

    def box(self, starts, row, octave, near, shift):
        lag = 2**octave
        boxes, shifted = [], []
        for run, z in near:
            pair = []
            for k in range(self.width + 2):
                total = z[k] + self.column(starts, run, k, row, shift)
                pair.append(total * (1.0 / lag) if octave else total)
            ahead = [pltpu.roll(v, LANES - lag, 1) for v in pair]
            if 2 * lag == LANES:
                plus = [
                    jnp.where(self.lane < lag, ahead[k], ahead[k + 1])
                    for k in range(self.width + 1)
                ]
                boxes += [pair[k + 1] + plus[k + 1] for k in range(self.width)]
                shifted += [pair[k + 1] + plus[k] for k in range(self.width)]
            else:
                behind = [pltpu.roll(v, lag, 1) for v in pair]
                for k in range(1, self.width + 1):
                    plus = jnp.where(self.lane < LANES - lag, ahead[k], ahead[k + 1])
                    minus = jnp.where(self.lane >= lag, behind[k], behind[k - 1])
                    boxes.append(pair[k] + plus)
                    shifted.append(pair[k] + minus)
        return boxes, shifted

    def add(self, lags, starts, row, run):
        near = self.near(starts, row, [run])
        count = self.width
        low = run * self.width
        first = second = None
        for octave in range(SCALES):
            shift = self.shift(octave)
            boxes, shifted = self.box(starts, row, octave, near, shift)
            here = row_pad(octave) + row
            for k in range(count):
                lags[octave][0, low + k, pl.ds(pl.multiple_of(here, SUB), SUB), :] = boxes[k]
                lags[octave][1, low + k, pl.ds(pl.multiple_of(here, SUB), SUB), :] = shifted[k]
            past = pl.ds(here - shift, SUB)
            u = [boxes[k] - lags[octave][1, low + k, past, :] for k in range(count)]
            v = [lags[octave][0, low + k, past, :] - shifted[k] for k in range(count)]
            first = u if first is None else [a + b for a, b in zip(first, u)]
            second = v if second is None else [a + b for a, b in zip(second, v)]
        return first, second

    def finish(self, starts, row, first, second, runs=(0, 1)):
        rows = pl.ds(pl.multiple_of(row, SUB), SUB)
        coef = self.coef[rows, :]
        turn = jnp.where(self.top, 1.0, -1.0) * (1.0 / (8.0 * SCALES))
        for k in range(len(runs) * self.width):
            run, within = runs[k // self.width], k % self.width
            column = pl.ds(pl.multiple_of((starts[run] + within) * LANES, LANES), LANES)
            grad_east = (first[k] + second[k]) * coef
            grad_north = (second[k] - first[k]) * turn
            squared = grad_east * grad_east + grad_north * grad_north
            inverse = lax.rsqrt(1.0 + squared)
            sine = squared * lax.rsqrt(jnp.maximum(squared, 1e-37)) * inverse
            ratio = jnp.full_like(inverse, ANGLE[-1])
            for term in ANGLE[-2::-1]:
                ratio = ratio * inverse + term
            self.slope[rows, column] = sine * ratio
            turned = -inverse
            self.facing[0, rows, column] = grad_east * turned
            self.facing[1, rows, column] = grad_north * turned
            tilt = 0.5 * (grad_east - grad_north) + LIGHT_UP
            self.shade[rows, column] = jnp.maximum(tilt * inverse, 0.0)


def run_starts(half, strips):
    quarter = strips // 4
    return (
        jnp.where(half == 0, quarter, 0),
        jnp.where(half == 0, 2 * quarter, 3 * quarter),
    )


def gather(rows, cols, z_ref, strips_ref, part, slope, facing, shade, *scratch):
    lags, (
        rim,
        far_rim,
        coef,
        greeted,
        load_sem,
        lat_send,
        lat_recv,
        send_sem,
        recv_sem,
        rim_send,
        rim_recv,
    ) = (
        scratch[:SCALES],
        scratch[SCALES:],
    )
    lat, lon = lax.axis_index("lat"), lax.axis_index("lon")
    n_lat, n_lon = lax.axis_size("lat"), lax.axis_size("lon")
    strips = cols // LANES
    hops = rim_hops(strips)
    width = strips // 4
    count = RUNS * width
    near = near_side(lat)
    far = 1 - near
    exists = (lat > 0, lat < n_lat - 1)
    far_exists = jnp.where(far == 0, exists[0], exists[1])
    far_lat = jnp.where(far == 0, lat - 1, lat + 1)
    near_lat = jnp.where(near == 0, lat - 1, lat + 1)

    def edge(side):
        return pl.multiple_of(jnp.where(side == 0, 0, rows - HALO), SUB)

    def halo(side):
        return pl.multiple_of(jnp.where(side == 0, 0, HALO + rows), SUB)

    def loads_of(number):
        start, size = ((edge(far), HALO), (edge(near), HALO), (HALO, rows - 2 * HALO))[number]
        return [
            pltpu.make_async_copy(
                z_ref.at[pl.ds(start, size), pl.ds(strip * LANES, LANES)],
                strips_ref.at[1 + strip, pl.ds(HALO + start, size), :],
                load_sem.at[number, strip],
            )
            for strip in range(strips)
        ]

    barrier = pltpu.get_barrier_semaphore()

    @pl.when(far_exists)
    def _():
        pl.semaphore_signal(barrier, inc=1, device_id=(far_lat, lon), device_id_type=MESH)

    pl.semaphore_signal(barrier, inc=1, device_id=(near_lat, lon), device_id_type=MESH)

    for number in range(3):
        for load in loads_of(number):
            load.start()

    main = rows - HALO
    base = pl.multiple_of(jnp.where(far == 0, HALO, 0), SUB)
    odd = lax.rem(lon, 2)
    leads = odd == 0
    follows = odd == 1
    pl.semaphore_wait(barrier, 1 + far_exists.astype(jnp.int32) + len(hops) * odd)

    @pl.when(leads)
    def _():
        for hop, _ in hops:
            pl.semaphore_signal(barrier, inc=1, device_id=(lat, hop), device_id_type=MESH)

    @pl.when(follows)
    def _():
        for hop, _ in hops:
            pl.semaphore_signal(greeted, inc=1, device_id=(lat, hop), device_id_type=MESH)


    pieces = ((1, 1), (strips, 1), (2, strips - 2))

    def lat_copy(distant, piece):
        side, other = (far, far_lat) if distant else (near, near_lat)
        part_ = pl.ds(*piece)
        index = pieces.index(piece)
        source = strips_ref.at[part_, pl.ds(HALO + edge(side), HALO), :]
        target = strips_ref.at[part_, pl.ds(halo(1 - side), HALO), :]
        if distant and piece[1] == 1:
            columns = pl.ds((piece[0] - 1) * LANES, LANES)
            source = z_ref.at[pl.ds(edge(side), HALO), columns]
            target = strips_ref.at[piece[0], pl.ds(halo(1 - side), HALO), :]
        return pltpu.make_async_remote_copy(
            src_ref=source,
            dst_ref=target,
            send_sem=lat_send.at[distant, index],
            recv_sem=lat_recv.at[distant, index],
            device_id=(other, lon),
            device_id_type=MESH,
        )

    def corner_copy(distant, index):
        hop, target = hops[index]
        source, row, other = (
            (far_rim, halo(far), lat) if distant else (rim, halo(far), near_lat)
        )
        source = source if distant else source.at[pl.ds(edge(near), HALO), :]
        return pltpu.make_async_remote_copy(
            src_ref=source,
            dst_ref=strips_ref.at[target, pl.ds(row, HALO), :],
            send_sem=send_sem.at[distant, index],
            recv_sem=recv_sem.at[distant, index],
            device_id=(other, hop),
            device_id_type=MESH,
        )

    def rim_copy(index, side):
        hop, target = hops[index]
        middle = rows // 2
        start = jnp.where((far if side == 0 else near) == 0, 0, middle)
        return pltpu.make_async_remote_copy(
            src_ref=rim.at[pl.ds(pl.multiple_of(start, SUB), middle), :],
            dst_ref=strips_ref.at[target, pl.ds(pl.multiple_of(HALO + start, SUB), middle), :],
            send_sem=rim_send.at[index, side],
            recv_sem=rim_recv.at[index, side],
            device_id=(lat, hop),
            device_id_type=MESH,
        )

    def arrived(distant, piece=None, index=0):
        here = pl.ds(halo(far if distant else near), HALO)
        if piece is None:
            place = strips_ref.at[hops[index][1], here, :]
            sends, receives = send_sem, recv_sem
        else:
            place = strips_ref.at[pl.ds(*piece), here, :]
            sends, receives, index = lat_send, lat_recv, pieces.index(piece)
        pltpu.make_async_remote_copy(
            src_ref=place,
            dst_ref=place,
            send_sem=sends.at[distant, index],
            recv_sem=receives.at[distant, index],
            device_id=(lat, hops[0][0]),
            device_id_type=MESH,
        ).wait_recv()

    @pl.when(far_exists)
    def _():
        for piece in pieces[:2]:
            lat_copy(1, piece).start()

    fill_coef(coef, main, lat * rows + base, rows * n_lat, cols * n_lon)
    for load in loads_of(0):
        load.wait()

    @pl.when(far_exists)
    def _():
        lat_copy(1, pieces[2]).start()

    for load in loads_of(1):
        load.wait()
    for piece in pieces:
        lat_copy(0, piece).start()
    for load in loads_of(2):
        load.wait()
    lane = lax.broadcasted_iota(jnp.int32, (SUB, LANES), 1)
    for start in range(0, rows, SUB):
        here = pl.ds(HALO + start, SUB)
        rim[pl.ds(start, SUB), :] = jnp.where(
            lane < HALO, strips_ref[1, here, :], strips_ref[strips, here, :]
        )

    for octave in range(SCALES):
        pad = row_pad(octave)
        first = pl.multiple_of(jnp.where(far == 0, 0, pad + rows), SUB)
        for k in range(count):
            for start in range(0, pad, SUB):
                for which in range(2):
                    lags[octave][which, k, pl.ds(first + start, SUB), :] = jnp.zeros(
                        (SUB, LANES), jnp.float32
                    )

    def send_rims():
        for index in range(len(hops)):
            for side in range(2):
                rim_copy(index, side).start()
            corner_copy(0, index).start()

    pl.when(follows)(send_rims)


    window = Window(strips_ref, rows, strips, far, coef, slope, facing, shade)
    far_base = pl.multiple_of(jnp.where(far == 0, 0, main), SUB)

    def half(number, carry):
        @pl.when(number == 1)
        def _():
            for index in range(len(hops)):
                rim_copy(index, 0).wait_recv()

        starts = run_starts(number, strips)

        def partly(block, carry):
            for inner in range(UNROLL):
                row = window.row(block * UNROLL + inner)
                rows_here = pl.ds(pl.multiple_of(row - far_base, SUB), SUB)
                for run in range(RUNS):
                    found = window.add(lags, starts, row, run)
                    for which in range(2):
                        for k in range(width):
                            part[which, starts[run] + k, rows_here, :] = found[which][k]
            return carry

        def fully(block, carry):
            for inner in range(UNROLL):
                row = window.row(block * UNROLL + inner)
                for run in range(RUNS):
                    window.finish(
                        starts, row - base, *window.add(lags, starts, row, run), runs=(run,)
                    )
            return carry

        size = UNROLL * SUB
        lax.fori_loop(0, HALO // size, partly, 0)

        @pl.when(jnp.logical_and(number == 0, leads))
        def _():
            pl.semaphore_wait(greeted, len(hops))
            send_rims()

        @pl.when(number == 1)
        def _():
            for index in range(len(hops)):
                rim_copy(index, 1).wait_recv()
                arrived(0, index=index)

        def segment(index, carry):
            outer = jnp.logical_and(number == 1, far_exists)

            @pl.when(jnp.logical_and(outer, index == 0))
            def _():
                for piece in pieces[:2]:
                    arrived(1, piece)
                for start in range(0, HALO, SUB):
                    here = pl.ds(pl.multiple_of(halo(far) + start, SUB), SUB)
                    far_rim[pl.ds(start, SUB), :] = jnp.where(
                        lane < HALO, strips_ref[1, here, :], strips_ref[strips, here, :]
                    )

            @pl.when(jnp.logical_and(outer, index == 1))
            def _():
                for hop in range(len(hops)):
                    corner_copy(1, hop).start()

            @pl.when(jnp.logical_and(number == 0, index == 2))
            def _():
                for piece in pieces:
                    arrived(0, piece)

            first, last, end = HALO // size, (rows - HALO) // size, rows // size
            low = jnp.where(index == 0, first, jnp.where(index == 1, first + 1, last))
            high = jnp.where(index == 0, first + 1, jnp.where(index == 1, last, end))
            lax.fori_loop(low, high, fully, 0)
            return carry

        lax.fori_loop(0, 3, segment, 0)
        return carry

    lax.fori_loop(0, 2, half, 0)

    for pole in range(2):

        @pl.when(jnp.logical_and(jnp.logical_not(far_exists), far == pole))
        def _():
            first = HALO if pole == 0 else HALO + rows - SUB
            pick = 0 if pole == 0 else SUB - 1
            fill = 0 if pole == 0 else HALO + rows

            def repeat(strip, carry):
                row = strips_ref[strip, pl.ds(first, SUB), :][pick : pick + 1]
                block = jnp.broadcast_to(row, (SUB, LANES))
                for k in range(HALO // SUB):
                    strips_ref[strip, pl.ds(fill + k * SUB, SUB), :] = block
                return carry

            lax.fori_loop(0, strips_ref.shape[0], repeat, 0)

    for piece in pieces:
        lat_copy(0, piece).wait_send()
    for index in range(len(hops)):
        for side in range(2):
            rim_copy(index, side).wait_send()
        corner_copy(0, index).wait_send()

    @pl.when(far_exists)
    def _():
        for piece in pieces:
            lat_copy(1, piece).wait_send()
        arrived(1, pieces[2])
        for index in range(len(hops)):
            corner_copy(1, index).wait_send()
            arrived(1, index=index)


def shade_far(rows, cols, *refs):
    strips_ref, part, slope, facing, shade, slope_out, facing_out, shade_out = refs[:8]
    coef, slope_far, facing_far, shade_far_, near_sem, far_sem = refs[8:]
    lat = lax.axis_index("lat")
    n_lat, n_lon = lax.axis_size("lat"), lax.axis_size("lon")
    far = 1 - near_side(lat)
    strips = cols // LANES
    width = strips // 4
    count = RUNS * width
    main = rows - HALO
    base = pl.multiple_of(jnp.where(far == 0, HALO, 0), SUB)
    far_base = pl.multiple_of(jnp.where(far == 0, 0, main), SUB)
    done = [
        pltpu.make_async_copy(source, target, near_sem.at[index])
        for index, (source, target) in enumerate(
            (
                (slope, slope_out.at[pl.ds(base, main), :]),
                (shade, shade_out.at[pl.ds(base, main), :]),
                (facing.at[0], facing_out.at[0, pl.ds(base, main), :]),
                (facing.at[1], facing_out.at[1, pl.ds(base, main), :]),
            )
        )
    ]
    for copy in done:
        copy.start()
    fill_coef(coef, HALO, lat * rows + far_base, rows * n_lat, cols * n_lon)
    window = Window(strips_ref, rows, strips, far, coef, slope_far, facing_far, shade_far_)
    sublane = lax.broadcasted_iota(jnp.int32, (SUB, LANES), 0)

    def copies(number):
        found = []
        for run, start in enumerate(run_starts(number, strips)):
            column = pl.ds(pl.multiple_of(start * LANES, LANES), width * LANES)
            here = pl.ds(far_base, HALO)
            for index, (source, target) in enumerate(
                (
                    (slope_far.at[:, column], slope_out.at[here, column]),
                    (shade_far_.at[:, column], shade_out.at[here, column]),
                    (facing_far.at[0, :, column], facing_out.at[0, here, column]),
                    (facing_far.at[1, :, column], facing_out.at[1, here, column]),
                )
            ):
                found.append(
                    pltpu.make_async_copy(source, target, far_sem.at[number, run, index])
                )
        return found

    def half(number, carry):
        starts = run_starts(number, strips)
        for step in range(HALO // SUB):
            row = window.row(step)
            local_row = pl.multiple_of(row - far_base, SUB)
            first, second = [
                [
                    part[which, starts[k // width] + k % width, pl.ds(local_row, SUB), :]
                    for k in range(count)
                ]
                for which in range(2)
            ]
            near = window.near(starts, row, range(RUNS))
            for octave in range(SCALES):
                lag = 2**octave
                if row_pad(octave) <= step * SUB:
                    continue
                boxes, shifted = window.box(starts, row, octave, near, -window.shift(octave))
                if lag < SUB:
                    beyond = jnp.logical_or(
                        jnp.logical_and(far == 0, sublane < lag),
                        jnp.logical_and(far == 1, sublane >= SUB - lag),
                    )
                    boxes = [jnp.where(beyond, v, 0.0) for v in boxes]
                    shifted = [jnp.where(beyond, v, 0.0) for v in shifted]
                first = [a - b for a, b in zip(first, shifted)]
                second = [a + b for a, b in zip(second, boxes)]
            window.finish(starts, local_row, first, second)
        for copy in copies(number):
            copy.start()
        return carry

    lax.fori_loop(0, 2, half, 0)
    for copy in done:
        copy.wait()
    for number in range(2):
        for copy in copies(number):
            copy.wait()


def local(elevation):
    rows, cols = elevation.shape
    strips = cols // LANES
    count = RUNS * (strips // 4)
    hops = 1 if lax.axis_size("lon") == 2 else 2
    main = rows - HALO
    vmem = pl.BlockSpec(memory_space=pltpu.VMEM)
    anywhere = pl.BlockSpec(memory_space=pl.ANY)
    staged = pl.pallas_call(
        functools.partial(gather, rows, cols),
        out_shape=(
            pltpu.VMEM((strips + hops, spread(rows + 2 * HALO), LANES), jnp.float32),
            pltpu.VMEM((2, strips, HALO, LANES), jnp.float32),
            pltpu.VMEM((main, cols), jnp.float32),
            pltpu.VMEM((2, main, cols), jnp.float32),
            pltpu.VMEM((main, cols), jnp.float32),
        ),
        in_specs=[anywhere],
        out_specs=(vmem,) * 5,
        scratch_shapes=[
            pltpu.VMEM((2, count, spread(rows + 2 * row_pad(k)), LANES), jnp.float32)
            for k in range(SCALES)
        ]
        + [
            pltpu.VMEM((rows, LANES), jnp.float32),
            pltpu.VMEM((HALO, LANES), jnp.float32),
            pltpu.VMEM((main, LANES), jnp.float32),
            pltpu.SemaphoreType.REGULAR,
            pltpu.SemaphoreType.DMA((3, strips)),
            pltpu.SemaphoreType.DMA((2, 3)),
            pltpu.SemaphoreType.DMA((2, 3)),
            pltpu.SemaphoreType.DMA((2, hops)),
            pltpu.SemaphoreType.DMA((2, hops)),
            pltpu.SemaphoreType.DMA((hops, 2)),
            pltpu.SemaphoreType.DMA((hops, 2)),
        ],
        compiler_params=pltpu.CompilerParams(
            collective_id=0, has_side_effects=True, vmem_limit_bytes=52 * 2**20
        ),
    )(elevation)
    return tuple(
        pl.pallas_call(
            functools.partial(shade_far, rows, cols),
            out_shape=(
                jax.ShapeDtypeStruct((rows, cols), jnp.float32),
                jax.ShapeDtypeStruct((2, rows, cols), jnp.float32),
                jax.ShapeDtypeStruct((rows, cols), jnp.float32),
            ),
            in_specs=[vmem] * 5,
            out_specs=(anywhere,) * 3,
            scratch_shapes=[
                pltpu.VMEM((HALO, LANES), jnp.float32),
                pltpu.VMEM((HALO, cols), jnp.float32),
                pltpu.VMEM((2, HALO, cols), jnp.float32),
                pltpu.VMEM((HALO, cols), jnp.float32),
                pltpu.SemaphoreType.DMA((4,)),
                pltpu.SemaphoreType.DMA((2, RUNS, 4)),
            ],
            compiler_params=pltpu.CompilerParams(vmem_limit_bytes=16 * 2**20),
        )(*staged)
    )


def solution(mesh):
    in_specs = (P("lat", "lon"),)
    out_specs = (P("lat", "lon"), P(None, "lat", "lon"), P("lat", "lon"))
    return jax.shard_map(local, mesh=mesh, in_specs=in_specs, out_specs=out_specs, check_vma=False)
```

```python
import functools
import math

import jax
import jax.numpy as jnp
from jax import lax
from jax.experimental import pallas as pl
from jax.experimental.pallas import tpu as pltpu
from jax.sharding import PartitionSpec as P

SCALES = 7
HALO = 64
LANES = 128
SUB = 8
RUNS = 2
UNROLL = 4

LIGHT_UP = math.sqrt(0.5)
MESH = pl.DeviceIdType.MESH

ANGLE = (
    1.5707962050889646,
    -0.9999801696091738,
    0.7848538132927688,
    -0.6607586188432167,
    0.5557489578459907,
    -0.42189571811945836,
    0.2501265286961767,
    -0.09607630454800326,
    0.01718536914918157,
)


def spread(rows):
    return rows + (-rows // SUB + 1) % 4 * SUB


def row_pad(octave):
    return max(2**octave, SUB)


def rim_hops(strips):
    lon, n_lon = lax.axis_index("lon"), lax.axis_size("lon")
    hops = [(lax.rem(lon + 1, n_lon), 0)]
    if n_lon > 2:
        hops.append((lax.rem(lon + n_lon - 1, n_lon), strips + 1))
    return hops


def east_halo(strips):
    return strips + 1 if lax.axis_size("lon") > 2 else 0


def near_side(lat):
    return 1 - lax.rem(lat, 2)


def fill_coef(coef_ref, count, first_row, total_rows, total_cols):
    row = lax.broadcasted_iota(jnp.int32, (SUB, LANES), 0)
    tile = jnp.minimum(lax.broadcasted_iota(jnp.int32, (SUB, LANES), 1), count // SUB - 1)
    position = first_row + row + tile * SUB
    spacing = jnp.sin((position.astype(jnp.float32) + 0.5) * (math.pi / total_rows)) * (
        2.0 * total_rows / total_cols
    )
    coef = 1.0 / (8.0 * SCALES * spacing)
    for number in range(count // SUB):
        coef_ref[pl.ds(number * SUB, SUB), :] = jnp.broadcast_to(
            coef[:, number : number + 1], (SUB, LANES)
        )


class Window:
    def __init__(self, strips, rows, columns, far, coef, slope, facing, shade):
        self.strips, self.rows, self.columns = strips, rows, columns
        self.width = columns // 4
        self.coef, self.slope, self.facing, self.shade = coef, slope, facing, shade
        self.top = far == 0
        self.sign = jnp.where(self.top, 1, -1)
        self.lane = lax.broadcasted_iota(jnp.int32, (SUB, LANES), 1)

    def row(self, number):
        return pl.multiple_of(
            jnp.where(self.top, number * SUB, self.rows - SUB - number * SUB), SUB
        )

    def shift(self, octave):
        lag = 2**octave
        moved = self.sign * lag
        return pl.multiple_of(moved, SUB) if lag >= SUB else moved

    def column(self, starts, run, offset, row, shift=0):
        place = pl.ds(HALO + row + shift, SUB)
        strip = starts[run] + offset
        if offset == self.width + 1:
            strip = jnp.where(strip > self.columns, east_halo(self.columns), strip)
        return self.strips[strip, place, :]

    def near(self, starts, row, runs):
        return [
            (run, [self.column(starts, run, k, row) for k in range(self.width + 2)])
            for run in runs
        ]

    def box(self, starts, row, octave, near, shift):
        lag = 2**octave
        boxes, shifted = [], []
        for run, z in near:
            pair = []
            for k in range(self.width + 2):
                total = z[k] + self.column(starts, run, k, row, shift)
                pair.append(total * (1.0 / lag) if octave else total)
            ahead = [pltpu.roll(v, LANES - lag, 1) for v in pair]
            if 2 * lag == LANES:
                plus = [
                    jnp.where(self.lane < lag, ahead[k], ahead[k + 1])
                    for k in range(self.width + 1)
                ]
                boxes += [pair[k + 1] + plus[k + 1] for k in range(self.width)]
                shifted += [pair[k + 1] + plus[k] for k in range(self.width)]
            else:
                behind = [pltpu.roll(v, lag, 1) for v in pair]
                for k in range(1, self.width + 1):
                    plus = jnp.where(self.lane < LANES - lag, ahead[k], ahead[k + 1])
                    minus = jnp.where(self.lane >= lag, behind[k], behind[k - 1])
                    boxes.append(pair[k] + plus)
                    shifted.append(pair[k] + minus)
        return boxes, shifted

    def add(self, lags, starts, row, run):
        near = self.near(starts, row, [run])
        count = self.width
        low = run * self.width
        first = second = None
        for octave in range(SCALES):
            shift = self.shift(octave)
            boxes, shifted = self.box(starts, row, octave, near, shift)
            here = row_pad(octave) + row
            for k in range(count):
                lags[octave][0, low + k, pl.ds(pl.multiple_of(here, SUB), SUB), :] = boxes[k]
                lags[octave][1, low + k, pl.ds(pl.multiple_of(here, SUB), SUB), :] = shifted[k]
            past = pl.ds(here - shift, SUB)
            u = [boxes[k] - lags[octave][1, low + k, past, :] for k in range(count)]
            v = [lags[octave][0, low + k, past, :] - shifted[k] for k in range(count)]
            first = u if first is None else [a + b for a, b in zip(first, u)]
            second = v if second is None else [a + b for a, b in zip(second, v)]
        return first, second

    def finish(self, starts, row, first, second, runs=(0, 1)):
        rows = pl.ds(pl.multiple_of(row, SUB), SUB)
        coef = self.coef[rows, :]
        turn = jnp.where(self.top, 1.0, -1.0) * (1.0 / (8.0 * SCALES))
        for k in range(len(runs) * self.width):
            run, within = runs[k // self.width], k % self.width
            column = pl.ds(pl.multiple_of((starts[run] + within) * LANES, LANES), LANES)
            grad_east = (first[k] + second[k]) * coef
            grad_north = (second[k] - first[k]) * turn
            squared = grad_east * grad_east + grad_north * grad_north
            inverse = lax.rsqrt(1.0 + squared)
            sine = squared * lax.rsqrt(jnp.maximum(squared, 1e-37)) * inverse
            ratio = jnp.full_like(inverse, ANGLE[-1])
            for term in ANGLE[-2::-1]:
                ratio = ratio * inverse + term
            self.slope[rows, column] = sine * ratio
            turned = -inverse
            self.facing[0, rows, column] = grad_east * turned
            self.facing[1, rows, column] = grad_north * turned
            tilt = 0.5 * (grad_east - grad_north) + LIGHT_UP
            self.shade[rows, column] = jnp.maximum(tilt * inverse, 0.0)


def run_starts(half, strips):
    quarter = strips // 4
    return (
        jnp.where(half == 0, quarter, 0),
        jnp.where(half == 0, 2 * quarter, 3 * quarter),
    )


def gather(rows, cols, z_ref, strips_ref, part, slope, facing, shade, *scratch):
    lags, (
        rim,
        far_rim,
        coef,
        greeted,
        load_sem,
        lat_send,
        lat_recv,
        send_sem,
        recv_sem,
        rim_send,
        rim_recv,
    ) = (
        scratch[:SCALES],
        scratch[SCALES:],
    )
    lat, lon = lax.axis_index("lat"), lax.axis_index("lon")
    n_lat, n_lon = lax.axis_size("lat"), lax.axis_size("lon")
    strips = cols // LANES
    hops = rim_hops(strips)
    width = strips // 4
    count = RUNS * width
    near = near_side(lat)
    far = 1 - near
    exists = (lat > 0, lat < n_lat - 1)
    far_exists = jnp.where(far == 0, exists[0], exists[1])
    far_lat = jnp.where(far == 0, lat - 1, lat + 1)
    near_lat = jnp.where(near == 0, lat - 1, lat + 1)

    def edge(side):
        return pl.multiple_of(jnp.where(side == 0, 0, rows - HALO), SUB)

    def halo(side):
        return pl.multiple_of(jnp.where(side == 0, 0, HALO + rows), SUB)

    def loads_of(number):
        start, size = ((edge(far), HALO), (edge(near), HALO), (HALO, rows - 2 * HALO))[number]
        return [
            pltpu.make_async_copy(
                z_ref.at[pl.ds(start, size), pl.ds(strip * LANES, LANES)],
                strips_ref.at[1 + strip, pl.ds(HALO + start, size), :],
                load_sem.at[number, strip],
            )
            for strip in range(strips)
        ]

    barrier = pltpu.get_barrier_semaphore()

    @pl.when(far_exists)
    def _():
        pl.semaphore_signal(barrier, inc=1, device_id=(far_lat, lon), device_id_type=MESH)

    pl.semaphore_signal(barrier, inc=1, device_id=(near_lat, lon), device_id_type=MESH)

    for number in range(3):
        for load in loads_of(number):
            load.start()

    main = rows - HALO
    base = pl.multiple_of(jnp.where(far == 0, HALO, 0), SUB)
    odd = lax.rem(lon, 2)
    leads = odd == 0
    follows = odd == 1
    pl.semaphore_wait(barrier, 1 + far_exists.astype(jnp.int32) + len(hops) * odd)

    @pl.when(leads)
    def _():
        for hop, _ in hops:
            pl.semaphore_signal(barrier, inc=1, device_id=(lat, hop), device_id_type=MESH)

    @pl.when(follows)
    def _():
        for hop, _ in hops:
            pl.semaphore_signal(greeted, inc=1, device_id=(lat, hop), device_id_type=MESH)


    pieces = ((1, 1), (strips, 1), (2, strips - 2))

    def lat_copy(distant, piece):
        side, other = (far, far_lat) if distant else (near, near_lat)
        part_ = pl.ds(*piece)
        index = pieces.index(piece)
        source = strips_ref.at[part_, pl.ds(HALO + edge(side), HALO), :]
        target = strips_ref.at[part_, pl.ds(halo(1 - side), HALO), :]
        if distant and piece[1] == 1:
            columns = pl.ds((piece[0] - 1) * LANES, LANES)
            source = z_ref.at[pl.ds(edge(side), HALO), columns]
            target = strips_ref.at[piece[0], pl.ds(halo(1 - side), HALO), :]
        return pltpu.make_async_remote_copy(
            src_ref=source,
            dst_ref=target,
            send_sem=lat_send.at[distant, index],
            recv_sem=lat_recv.at[distant, index],
            device_id=(other, lon),
            device_id_type=MESH,
        )

    def corner_copy(distant, index):
        hop, target = hops[index]
        source, row, other = (
            (far_rim, halo(far), lat) if distant else (rim, halo(far), near_lat)
        )
        source = source if distant else source.at[pl.ds(edge(near), HALO), :]
        return pltpu.make_async_remote_copy(
            src_ref=source,
            dst_ref=strips_ref.at[target, pl.ds(row, HALO), :],
            send_sem=send_sem.at[distant, index],
            recv_sem=recv_sem.at[distant, index],
            device_id=(other, hop),
            device_id_type=MESH,
        )

    def rim_copy(index, side):
        hop, target = hops[index]
        middle = rows // 2
        start = jnp.where((far if side == 0 else near) == 0, 0, middle)
        return pltpu.make_async_remote_copy(
            src_ref=rim.at[pl.ds(pl.multiple_of(start, SUB), middle), :],
            dst_ref=strips_ref.at[target, pl.ds(pl.multiple_of(HALO + start, SUB), middle), :],
            send_sem=rim_send.at[index, side],
            recv_sem=rim_recv.at[index, side],
            device_id=(lat, hop),
            device_id_type=MESH,
        )

    def arrived(distant, piece=None, index=0):
        here = pl.ds(halo(far if distant else near), HALO)
        if piece is None:
            place = strips_ref.at[hops[index][1], here, :]
            sends, receives = send_sem, recv_sem
        else:
            place = strips_ref.at[pl.ds(*piece), here, :]
            sends, receives, index = lat_send, lat_recv, pieces.index(piece)
        pltpu.make_async_remote_copy(
            src_ref=place,
            dst_ref=place,
            send_sem=sends.at[distant, index],
            recv_sem=receives.at[distant, index],
            device_id=(lat, hops[0][0]),
            device_id_type=MESH,
        ).wait_recv()

    @pl.when(far_exists)
    def _():
        for piece in pieces[:2]:
            lat_copy(1, piece).start()

    fill_coef(coef, main, lat * rows + base, rows * n_lat, cols * n_lon)
    for load in loads_of(0):
        load.wait()

    @pl.when(far_exists)
    def _():
        lat_copy(1, pieces[2]).start()

    for load in loads_of(1):
        load.wait()
    for piece in pieces:
        lat_copy(0, piece).start()
    for load in loads_of(2):
        load.wait()
    lane = lax.broadcasted_iota(jnp.int32, (SUB, LANES), 1)
    for start in range(0, rows, SUB):
        here = pl.ds(HALO + start, SUB)
        rim[pl.ds(start, SUB), :] = jnp.where(
            lane < HALO, strips_ref[1, here, :], strips_ref[strips, here, :]
        )

    for octave in range(SCALES):
        pad = row_pad(octave)
        first = pl.multiple_of(jnp.where(far == 0, 0, pad + rows), SUB)
        for k in range(count):
            for start in range(0, pad, SUB):
                for which in range(2):
                    lags[octave][which, k, pl.ds(first + start, SUB), :] = jnp.zeros(
                        (SUB, LANES), jnp.float32
                    )

    def send_rims():
        for index in range(len(hops)):
            for side in range(2):
                rim_copy(index, side).start()
            corner_copy(0, index).start()

    pl.when(follows)(send_rims)


    window = Window(strips_ref, rows, strips, far, coef, slope, facing, shade)
    far_base = pl.multiple_of(jnp.where(far == 0, 0, main), SUB)

    def half(number, carry):
        @pl.when(number == 1)
        def _():
            for index in range(len(hops)):
                rim_copy(index, 0).wait_recv()

        starts = run_starts(number, strips)

        def partly(block, carry):
            for inner in range(UNROLL):
                row = window.row(block * UNROLL + inner)
                rows_here = pl.ds(pl.multiple_of(row - far_base, SUB), SUB)
                for run in range(RUNS):
                    found = window.add(lags, starts, row, run)
                    for which in range(2):
                        for k in range(width):
                            part[which, starts[run] + k, rows_here, :] = found[which][k]
            return carry

        def fully(block, carry):
            for inner in range(UNROLL):
                row = window.row(block * UNROLL + inner)
                for run in range(RUNS):
                    window.finish(
                        starts, row - base, *window.add(lags, starts, row, run), runs=(run,)
                    )
            return carry

        size = UNROLL * SUB
        lax.fori_loop(0, HALO // size, partly, 0)

        @pl.when(jnp.logical_and(number == 0, leads))
        def _():
            pl.semaphore_wait(greeted, len(hops))
            send_rims()

        @pl.when(number == 1)
        def _():
            for index in range(len(hops)):
                rim_copy(index, 1).wait_recv()
                arrived(0, index=index)

        def segment(index, carry):
            outer = jnp.logical_and(number == 1, far_exists)

            @pl.when(jnp.logical_and(outer, index == 0))
            def _():
                for piece in pieces[:2]:
                    arrived(1, piece)
                for start in range(0, HALO, SUB):
                    here = pl.ds(pl.multiple_of(halo(far) + start, SUB), SUB)
                    far_rim[pl.ds(start, SUB), :] = jnp.where(
                        lane < HALO, strips_ref[1, here, :], strips_ref[strips, here, :]
                    )

            @pl.when(jnp.logical_and(outer, index == 1))
            def _():
                for hop in range(len(hops)):
                    corner_copy(1, hop).start()

            @pl.when(jnp.logical_and(number == 0, index == 2))
            def _():
                for piece in pieces:
                    arrived(0, piece)

            first, last, end = HALO // size, (rows - HALO) // size, rows // size
            low = jnp.where(index == 0, first, jnp.where(index == 1, first + 1, last))
            high = jnp.where(index == 0, first + 1, jnp.where(index == 1, last, end))
            lax.fori_loop(low, high, fully, 0)
            return carry

        lax.fori_loop(0, 3, segment, 0)
        return carry

    lax.fori_loop(0, 2, half, 0)

    for pole in range(2):

        @pl.when(jnp.logical_and(jnp.logical_not(far_exists), far == pole))
        def _():
            first = HALO if pole == 0 else HALO + rows - SUB
            pick = 0 if pole == 0 else SUB - 1
            fill = 0 if pole == 0 else HALO + rows

            def repeat(strip, carry):
                row = strips_ref[strip, pl.ds(first, SUB), :][pick : pick + 1]
                block = jnp.broadcast_to(row, (SUB, LANES))
                for k in range(HALO // SUB):
                    strips_ref[strip, pl.ds(fill + k * SUB, SUB), :] = block
                return carry

            lax.fori_loop(0, strips_ref.shape[0], repeat, 0)

    for piece in pieces:
        lat_copy(0, piece).wait_send()
    for index in range(len(hops)):
        for side in range(2):
            rim_copy(index, side).wait_send()
        corner_copy(0, index).wait_send()

    @pl.when(far_exists)
    def _():
        for piece in pieces:
            lat_copy(1, piece).wait_send()
        arrived(1, pieces[2])
        for index in range(len(hops)):
            corner_copy(1, index).wait_send()
            arrived(1, index=index)


def shade_far(rows, cols, *refs):
    strips_ref, part, slope, facing, shade, slope_out, facing_out, shade_out = refs[:8]
    coef, slope_far, facing_far, shade_far_, near_sem, far_sem = refs[8:]
    lat = lax.axis_index("lat")
    n_lat, n_lon = lax.axis_size("lat"), lax.axis_size("lon")
    far = 1 - near_side(lat)
    strips = cols // LANES
    width = strips // 4
    count = RUNS * width
    main = rows - HALO
    base = pl.multiple_of(jnp.where(far == 0, HALO, 0), SUB)
    far_base = pl.multiple_of(jnp.where(far == 0, 0, main), SUB)
    done = [
        pltpu.make_async_copy(source, target, near_sem.at[index])
        for index, (source, target) in enumerate(
            (
                (slope, slope_out.at[pl.ds(base, main), :]),
                (shade, shade_out.at[pl.ds(base, main), :]),
                (facing, facing_out.at[:, pl.ds(base, main), :]),
            )
        )
    ]
    for copy in done:
        copy.start()
    fill_coef(coef, HALO, lat * rows + far_base, rows * n_lat, cols * n_lon)
    window = Window(strips_ref, rows, strips, far, coef, slope_far, facing_far, shade_far_)
    sublane = lax.broadcasted_iota(jnp.int32, (SUB, LANES), 0)

    def copies(number):
        found = []
        for run, start in enumerate(run_starts(number, strips)):
            column = pl.ds(pl.multiple_of(start * LANES, LANES), width * LANES)
            here = pl.ds(far_base, HALO)
            for index, (source, target) in enumerate(
                (
                    (slope_far.at[:, column], slope_out.at[here, column]),
                    (shade_far_.at[:, column], shade_out.at[here, column]),
                    (facing_far.at[:, :, column], facing_out.at[:, here, column]),
                )
            ):
                found.append(
                    pltpu.make_async_copy(source, target, far_sem.at[number, run, index])
                )
        return found

    def half(number, carry):
        starts = run_starts(number, strips)
        for step in range(HALO // SUB):
            row = window.row(step)
            local_row = pl.multiple_of(row - far_base, SUB)
            first, second = [
                [
                    part[which, starts[k // width] + k % width, pl.ds(local_row, SUB), :]
                    for k in range(count)
                ]
                for which in range(2)
            ]
            near = window.near(starts, row, range(RUNS))
            for octave in range(SCALES):
                lag = 2**octave
                if row_pad(octave) <= step * SUB:
                    continue
                boxes, shifted = window.box(starts, row, octave, near, -window.shift(octave))
                if lag < SUB:
                    beyond = jnp.logical_or(
                        jnp.logical_and(far == 0, sublane < lag),
                        jnp.logical_and(far == 1, sublane >= SUB - lag),
                    )
                    boxes = [jnp.where(beyond, v, 0.0) for v in boxes]
                    shifted = [jnp.where(beyond, v, 0.0) for v in shifted]
                first = [a - b for a, b in zip(first, shifted)]
                second = [a + b for a, b in zip(second, boxes)]
            window.finish(starts, local_row, first, second)
        for copy in copies(number):
            copy.start()
        return carry

    lax.fori_loop(0, 2, half, 0)
    for copy in done:
        copy.wait()
    for number in range(2):
        for copy in copies(number):
            copy.wait()


def local(elevation):
    rows, cols = elevation.shape
    strips = cols // LANES
    count = RUNS * (strips // 4)
    hops = 1 if lax.axis_size("lon") == 2 else 2
    main = rows - HALO
    vmem = pl.BlockSpec(memory_space=pltpu.VMEM)
    anywhere = pl.BlockSpec(memory_space=pl.ANY)
    staged = pl.pallas_call(
        functools.partial(gather, rows, cols),
        out_shape=(
            pltpu.VMEM((strips + hops, spread(rows + 2 * HALO), LANES), jnp.float32),
            pltpu.VMEM((2, strips, HALO, LANES), jnp.float32),
            pltpu.VMEM((main, cols), jnp.float32),
            pltpu.VMEM((2, main, cols), jnp.float32),
            pltpu.VMEM((main, cols), jnp.float32),
        ),
        in_specs=[anywhere],
        out_specs=(vmem,) * 5,
        scratch_shapes=[
            pltpu.VMEM((2, count, spread(rows + 2 * row_pad(k)), LANES), jnp.float32)
            for k in range(SCALES)
        ]
        + [
            pltpu.VMEM((rows, LANES), jnp.float32),
            pltpu.VMEM((HALO, LANES), jnp.float32),
            pltpu.VMEM((main, LANES), jnp.float32),
            pltpu.SemaphoreType.REGULAR,
            pltpu.SemaphoreType.DMA((3, strips)),
            pltpu.SemaphoreType.DMA((2, 3)),
            pltpu.SemaphoreType.DMA((2, 3)),
            pltpu.SemaphoreType.DMA((2, hops)),
            pltpu.SemaphoreType.DMA((2, hops)),
            pltpu.SemaphoreType.DMA((hops, 2)),
            pltpu.SemaphoreType.DMA((hops, 2)),
        ],
        compiler_params=pltpu.CompilerParams(
            collective_id=0, has_side_effects=True, vmem_limit_bytes=52 * 2**20
        ),
    )(elevation)
    return tuple(
        pl.pallas_call(
            functools.partial(shade_far, rows, cols),
            out_shape=(
                jax.ShapeDtypeStruct((rows, cols), jnp.float32),
                jax.ShapeDtypeStruct((2, rows, cols), jnp.float32),
                jax.ShapeDtypeStruct((rows, cols), jnp.float32),
            ),
            in_specs=[vmem] * 5,
            out_specs=(anywhere,) * 3,
            scratch_shapes=[
                pltpu.VMEM((HALO, LANES), jnp.float32),
                pltpu.VMEM((HALO, cols), jnp.float32),
                pltpu.VMEM((2, HALO, cols), jnp.float32),
                pltpu.VMEM((HALO, cols), jnp.float32),
                pltpu.SemaphoreType.DMA((3,)),
                pltpu.SemaphoreType.DMA((2, RUNS, 3)),
            ],
            compiler_params=pltpu.CompilerParams(vmem_limit_bytes=16 * 2**20),
        )(*staged)
    )


def solution(mesh):
    in_specs = (P("lat", "lon"),)
    out_specs = (P("lat", "lon"), P(None, "lat", "lon"), P("lat", "lon"))
    return jax.shard_map(local, mesh=mesh, in_specs=in_specs, out_specs=out_specs, check_vma=False)
```
